32 devices in a mesh: dp: 4 (over z), row: 2 (over y), col: 4 (over x, core).
Axes of the slice: x: 2, y: 2, z: 4, core: 2. Of those that a mesh axis runs over, the one named last changes fastest.
Arguments:
- activations: bfloat16 [4096, 4096], P('dp', 'col'), may hold values from -6 to 6
- out_grad: bfloat16 [4096, 14336], P('dp', 'row'), may hold values from -6 to 6
- weight: float32 [2, 7168, 4096], P('row', 'dp', 'col'), as said below
- step_size: float32 [2, 7168], P('row'), may hold values from 0.001 to 0.016
Outputs:
- input_grad: bfloat16 [4096, 4096], P(('dp', 'row'), 'col')
- weight_grad: float32 [2, 7168, 4096], P('row', 'dp', 'col')
- step_grad: float32 [2, 7168], P('row', 'dp')
The draws below stay inside these ranges and needn't reach their ends.
Inputs may be any that keep to these rules, and one draw needn't show every extreme that they name: Each latent weight divided by its row's step lies at least 0.1 away from every multiple of one half.
All inputs are finite; a program needn't handle non-finite values.
Results may differ from the reference program's by a relative error of at most 0.0096.
Values may be sent and summed in bfloat16 or wider, within the bound.
A program may use at most 128 MiB of HBM per device.

```python
import jax
import jax.numpy as jnp
from jax import lax

D = 4096
FF = 14336
TOKENS = 4096
N_ROW = 2


def joint_draw(key):
    base = jax.random.fold_in(key, 7)
    first, second, third, fourth = jax.random.split(base, 4)
    logs = jax.random.uniform(first, (N_ROW, FF // N_ROW), jnp.float32, jnp.log(0.002), jnp.log(0.008))
    scales = jnp.exp(logs)
    codes = jax.random.randint(second, (N_ROW, FF // N_ROW, D), -10, 10).astype(jnp.float32)
    magnitudes = jax.random.uniform(third, (N_ROW, FF // N_ROW, D), jnp.float32, 0.1, 0.4)
    signs = jnp.where(jax.random.bernoulli(fourth, 0.5, (N_ROW, FF // N_ROW, D)), 1.0, -1.0)
    latent = scales[:, :, None] * (codes + signs * magnitudes)
    return (scales, latent)


def draw_weight(key, part):
    scales, latent = joint_draw(key)
    return latent.astype(jnp.float32)


def draw_step_size(key, part):
    scales, latent = joint_draw(key)
    return scales.astype(jnp.float32)


def with_spikes(values, own_key, source, target, blocks, factor):
    owner, partner = [(jnp.arange(values.shape[position]) // (values.shape[position] // blocks)).reshape([-1 if axis == position else 1 for axis in range(values.ndim)]) for position in (source, target)]
    chosen = jax.random.permutation(own_key, blocks)[partner]
    strong = (owner == chosen) | (owner == (partner + blocks // 2) % blocks)
    return jnp.where(strong, factor * values, values)


def level_of(stream_key, shape, shards, smallest, top_value):
    def one(axis_at, shards_of):
        heights = jax.random.uniform(jax.random.fold_in(jax.random.fold_in(stream_key, 6), axis_at), (shards_of,), jnp.float32, smallest / len(shards), top_value / len(shards))
        return jnp.repeat(jnp.exp(heights), shape[axis_at] // shards_of).reshape((-1,) + (1,) * (len(shape) - axis_at - 1))

    level = one(*shards[0])
    for cut in shards[1:]:
        level = level * one(*cut)
    return level


def noise(key, dims, spread, bound, cuts=(), held_as=jnp.bfloat16):
    entries = jax.random.normal(key, dims, jnp.float32) * spread
    if len(cuts) > 0:
        entries = level_of(key, dims, cuts, -0.22, 0.18) * entries
    return jnp.clip(entries, min=-bound, max=bound).astype(held_as)


def heavy_noise(key, dims, spread, limit, shards, heavy, held_as=jnp.bfloat16):
    drawn = spread * jax.random.normal(key, dims, jnp.float32)
    if shards:
        drawn = drawn * level_of(key, dims, shards, -0.22, 0.18)
    return jnp.clip(with_spikes(drawn, jax.random.fold_in(key, 3), *heavy), -limit, limit).astype(held_as)


def setup_inputs(seed: int = 0) -> dict:
    arg_keys = jax.random.split(jax.random.key(seed), 5)
    activations = noise(arg_keys[0], (TOKENS, D), 1.0, 6.0, ((0, 4), (1, 4)))
    out_grad = heavy_noise(arg_keys[1], (TOKENS, FF), ((D / FF) ** 0.5), 6.0, ((0, 4), (1, 2)), (0, 1, 4, 2.0))
    weight = draw_weight(jax.random.fold_in(arg_keys[4], 71), 0)
    step_size = draw_step_size(jax.random.fold_in(arg_keys[4], 71), 0)
    return dict(activations=activations, out_grad=out_grad, weight=weight, step_size=step_size)


def reference(activations, out_grad, weight, step_size):
    scales = step_size.reshape(FF)
    latent = weight.reshape(FF, D)
    ratio = latent / scales[:, None]
    clipped = jnp.clip(ratio, -8.0, 7.0)
    levels = jnp.floor(clipped + 0.5)
    quantized = (levels * scales[:, None]).astype(jnp.bfloat16)
    inside = jnp.where((ratio >= -8.0) & (ratio <= 7.0), 1.0, 0.0).astype(jnp.float32)
    factor = jnp.where(inside > 0.5, levels - ratio, clipped)
    input_grad = jnp.dot(out_grad, quantized, preferred_element_type=jnp.float32).astype(jnp.bfloat16)
    products = lax.dot_general(out_grad, activations, (((0,), (0,)), ((), ())), preferred_element_type=jnp.float32)
    weight_grad = (products * inside).reshape(N_ROW, FF // N_ROW, D)
    grad_factor = 1.0 / (7.0 * D) ** 0.5
    step_grad = (jnp.sum(products * factor, axis=1) * grad_factor).reshape(N_ROW, FF // N_ROW)
    return input_grad, weight_grad, step_grad
```

```python
import jax
import jax.numpy as jnp
from jax import lax
from jax.experimental.layout import Layout, with_layout_constraint
from jax.experimental import pallas as pl
from jax.experimental.pallas import tpu as pltpu
from jax.sharding import PartitionSpec as P

D = 4096


def quantize(latent, scales):
    ratio = latent / scales[:, None]
    clipped = jnp.clip(ratio, -8.0, 7.0)
    levels = jnp.floor(clipped + 0.5)
    inside = jnp.where((ratio >= -8.0) & (ratio <= 7.0), 1.0, 0.0).astype(jnp.float32)
    factor = jnp.where(inside > 0.5, levels - ratio, clipped)
    quantized = (levels * scales[:, None]).astype(jnp.bfloat16)
    return (quantized, inside, factor)


def shift(block, axis, count, by):
    return lax.ppermute(block, axis, [(i, (i + by) % count) for i in range(count)])


def swap(block, axis, count, bit):
    return lax.ppermute(block, axis, [(i, i ^ bit) for i in range(count)])


def gather_rows(block, axis, count):
    position = lax.axis_index(axis)
    bit = 1
    bits = []
    while bit < count:
        bits.append(bit)
        bit *= 2
    pieces = {0: block}
    for bit in reversed(bits):
        held = dict(pieces)
        for key in held:
            pieces[key ^ bit] = swap(held[key], axis, count, bit)
    parts = [pieces[key] for key in range(count)]
    for bit in bits:
        flag = (position & bit) != 0
        parts = [
            jnp.where(flag, parts[key ^ bit], parts[key]) for key in range(count)
        ]
    return jnp.concatenate(parts, axis=0)


def make_shards(n_dp, n_row, n_col):
    def shards(activations, out_grad, weight, step_size):
        own_count = weight.shape[1]
        tokens = out_grad.shape[0]
        dp = lax.axis_index("dp")
        row = lax.axis_index("row")
        col = lax.axis_index("col")
        scales = step_size[0]
        own_scales = lax.dynamic_slice_in_dim(scales, dp * own_count, own_count, 0)
        grad_factor = 1.0 / (7.0 * D) ** 0.5

        share = tokens // n_col
        half = tokens // n_row
        mine = lax.dynamic_slice_in_dim(out_grad, col * share, share, 0)
        ring = lax.dynamic_slice_in_dim(activations, row * half, half, 0)
        grads, acts = [], []
        for k in range(1, n_dp):
            target = (dp + k) % n_dp
            chunk = lax.dynamic_slice_in_dim(mine, target * own_count, own_count, 1)
            grads.append(shift(chunk, "dp", n_dp, k))
            ring = shift(ring, "dp", n_dp, 1)
            acts.append(ring)

        quantized, _, _ = quantize(weight[0], own_scales)
        own_grad = lax.dynamic_slice_in_dim(out_grad, dp * own_count, own_count, 1)

        def reduced(grad):
            size = tokens
            bit = n_row // 2
            if bit == 0:
                return jnp.dot(grad, quantized, preferred_element_type=jnp.float32)
            size //= 2
            upper = ((row // bit) % 2).astype(jnp.int32)
            sent = lax.dynamic_slice_in_dim(grad, (1 - upper) * size, size, 0)
            kept = lax.dynamic_slice_in_dim(grad, upper * size, size, 0)
            out = jnp.dot(sent, quantized, preferred_element_type=jnp.float32).astype(jnp.bfloat16)
            came = swap(out, "row", n_row, bit)
            total = jnp.dot(kept, quantized, preferred_element_type=jnp.float32) + came.astype(jnp.float32)
            bit //= 2
            while bit:
                size //= 2
                upper = (row // bit) % 2 == 1
                low, high = total[:size], total[size:]
                came = swap(jnp.where(upper, low, high).astype(jnp.bfloat16), "row", n_row, bit)
                total = jnp.where(upper, high, low) + came.astype(jnp.float32)
                bit //= 2
            return total

        products = lax.dot_general(
            own_grad, activations, (((0,), (0,)), ((), ())), preferred_element_type=jnp.float32
        )
        own_total = reduced(own_grad)
        if grads:
            grads[0], quantized, products = lax.optimization_barrier((grads[0], quantized, products))
        running = None
        for k in range(1, n_dp):
            grad = gather_rows(grads[k - 1], "col", n_col)
            total = reduced(grad)
            if running is not None:
                total = total + running.astype(jnp.float32)
            leaving, grad = lax.optimization_barrier((total.astype(jnp.bfloat16), grad))
            running = shift(leaving, "dp", n_dp, 1)
            act = gather_rows(acts[k - 1], "row", n_row)
            products = products + lax.dot_general(
                grad, act, (((0,), (0,)), ((), ())), preferred_element_type=jnp.float32
            )
        if running is not None:
            own_total = own_total + running.astype(jnp.float32)
        products, latent = lax.optimization_barrier((products, weight[0]))
        products = with_layout_constraint(products, Layout((0, 1)))
        _, inside, factor = quantize(latent, own_scales)
        input_grad = own_total.astype(jnp.bfloat16)
        step_rows = lax.psum(jnp.sum(products * factor, axis=1) * grad_factor, "col")
        weight_grad = (products * inside)[None]
        return (input_grad, weight_grad, step_rows[None])

    return shards


MESH = pl.DeviceIdType.MESH


def flipped(position, bit):
    return position + bit * (1 - 2 * lax.rem(position // bit, 2))


def make_kernel(n_dp, n_row, n_col, tokens, own, width):
    quarter = tokens // n_col
    half = tokens // n_row
    piece = 128
    pieces = half // piece
    block = 256
    factor_scale = 1.0 / (7.0 * width * n_col) ** 0.5
    bits = []
    bit = n_col // 2
    while bit:
        bits.append(bit)
        bit //= 2

    def kernel(act, out_grad, weight, steps, input_grad, weight_grad, step_grad,
               g_buf, a_buf, q_buf, prod, p_send, p_recv, c_send, c_recv, w_buf, s_buf, acc, sg_buf, sg_in,
               load_sem, w_sem, out_sem, gz_send, g_recv, gx_send, az_send, ay_send, a_recv,
               p_ssem, p_rsem, c_ssem, c_rsem, sg_ssem, sg_rsem):
        me = lax.axis_index("dp")
        row = lax.axis_index("row")
        col = lax.axis_index("col")
        partner = 1 - row

        def remote(src, dst, send, recv, where):
            return pltpu.make_async_remote_copy(
                src_ref=src, dst_ref=dst, send_sem=send, recv_sem=recv, device_id=where, device_id_type=MESH
            )

        def rows_of(index, size):
            return pl.ds(pl.multiple_of(index * size, size), size)

        barrier = pltpu.get_barrier_semaphore()
        for k in range(1, n_dp):
            pl.semaphore_signal(barrier, inc=1, device_id={"dp": lax.rem(me + k, n_dp)}, device_id_type=MESH)
        pl.semaphore_signal(barrier, inc=1, device_id={"row": partner}, device_id_type=MESH)
        for bit in bits:
            pl.semaphore_signal(barrier, inc=1, device_id={"col": flipped(col, bit)}, device_id_type=MESH)

        own_columns = pl.ds(pl.multiple_of(me * own, 128), own)
        load_g = pltpu.make_async_copy(out_grad.at[:, own_columns], g_buf.at[me], load_sem.at[0])
        load_a = pltpu.make_async_copy(act, a_buf.at[me], load_sem.at[1])

        def load_w(k):
            return pltpu.make_async_copy(weight.at[0, pl.ds(k * block, block)], w_buf.at[k % 2], w_sem.at[k % 2])

        load_w(0).start()
        load_w(1).start()
        load_g.start()
        load_a.start()
        pl.semaphore_wait(barrier, n_dp - 1 + 1 + len(bits))

        def send_g(target):
            columns = pl.ds(pl.multiple_of(target * own, 128), own)
            return remote(
                out_grad.at[rows_of(col, quarter), columns], g_buf.at[me, rows_of(col, quarter)],
                gz_send.at[target], g_recv.at[me, col], {"dp": target},
            )

        def each_target(fn):
            for dist in range(1, n_dp):
                @pl.when(me + dist < n_dp)
                def _():
                    fn(me + dist)

                @pl.when(me - dist >= 0)
                def _():
                    fn(me - dist)

        each_target(lambda t: send_g(t).start())

        def send_a(source, toward):
            part = rows_of(row, half)
            origin = act.at[part] if source is None else a_buf.at[source, part]
            index = me if source is None else source
            return remote(
                origin, a_buf.at[index, part], az_send.at[index, (toward + 1) // 2], a_recv.at[index, row],
                {"dp": me + toward},
            )

        def swap_a(source):
            part = rows_of(row, half)
            return remote(
                a_buf.at[source, part], a_buf.at[source, part], ay_send.at[source], a_recv.at[source, row], {"row": partner}
            )

        def arrived_a(source, which):
            part = rows_of(which, half)
            remote(
                a_buf.at[source, part], a_buf.at[source, part], ay_send.at[source], a_recv.at[source, which], {"row": partner}
            ).wait_recv()

        @pl.when(me < n_dp - 1)
        def _():
            send_a(None, 1).start()

        @pl.when(me > 0)
        def _():
            send_a(None, -1).start()

        for k in range(own // 128):
            values = steps[0:1, pl.ds(pl.multiple_of(me * own + k * 128, 128), 128)]
            s_buf[pl.ds(k * 128, 128), :] = jnp.transpose(jnp.broadcast_to(values, (128, 128)))

        n_block = own // block

        def ratio_of(k):
            s = jnp.concatenate([s_buf[pl.ds(k * block, block), :]] * (width // 128), axis=1)
            return w_buf[k % 2] / s, s

        for k in range(n_block):
            load_w(k).wait()
            ratio, s = ratio_of(k)
            levels = jnp.floor(jnp.clip(ratio, -8.0, 7.0) + 0.5)
            q_buf[pl.ds(k * block, block), :] = (levels * s).astype(jnp.bfloat16)
            if k + 2 < n_block:
                load_w(k + 2).start()
        load_g.wait()

        def dx_tile(d, start, size):
            return jnp.dot(
                g_buf[d, pl.ds(pl.multiple_of(start, size), size), :], q_buf[...], preferred_element_type=jnp.float32
            )

        def partial(d, i):
            part = pl.ds(pl.multiple_of(i * piece, piece), piece)
            return remote(p_send.at[d, part], p_recv.at[d, part], p_ssem.at[d, i], p_rsem.at[d, i], {"row": partner})

        def send_partials(d):
            def body(i, carry):
                p_send[d, pl.ds(pl.multiple_of(i * piece, piece), piece), :] = dx_tile(
                    d, partner * half + i * piece, piece
                ).astype(jnp.bfloat16)
                partial(d, i).start()
                return carry

            lax.fori_loop(0, pieces, body, 0)

        def add_products(d, first=False):
            def body(k, carry):
                rows = pl.ds(pl.multiple_of(k * block, block), block)
                new = lax.dot_general(
                    g_buf[d, :, rows], a_buf[d], (((0,), (0,)), ((), ())), preferred_element_type=jnp.float32
                )
                if first:
                    prod[rows, :] = new
                else:
                    prod[rows, :] = new + prod[rows, :]
                return carry

            lax.fori_loop(0, n_block, body, 0)

        send_partials(me)
        load_a.wait()

        upper = me // (n_dp // 2)
        mirrored = me + upper * (n_dp - 1 - 2 * me)

        def nth(s):
            d = s + (s - mirrored + n_dp) // n_dp
            return d + upper * (n_dp - 1 - 2 * d)

        def g_part(d, which):
            return g_buf.at[d, rows_of(which, quarter)]

        def forward_g(d, which, b, slot):
            return remote(
                g_part(d, which), g_part(d, which), gx_send.at[d, slot], g_recv.at[d, which], {"col": flipped(col, bits[b])}
            )

        def arrived_g(d, which):
            remote(
                g_part(d, which), g_part(d, which), gx_send.at[d, 0], g_recv.at[d, which], {"col": flipped(col, bits[0])}
            ).wait_recv()

        def hypercube(d, on_arrival, on_send):
            slot = 0
            held = [col]
            on_arrival(d, col)
            for b in range(len(bits)):
                on_send(d, col, b, slot)
                slot += 1
            for b in range(len(bits)):
                come = [flipped(which, bits[b]) for which in held]
                for which in come:
                    on_arrival(d, which)
                    for later in range(b + 1, len(bits)):
                        on_send(d, which, later, slot)
                        slot += 1
                held += come

        for s in range(n_dp - 1):
            d = nth(s)
            hypercube(d, arrived_g, lambda *a: forward_g(*a).start())
            send_partials(d)
            if s == 0:
                add_products(me, first=True)

        def chain(d, slot, i, toward):
            part = pl.ds(pl.multiple_of(i * piece, piece), piece)
            return remote(c_send.at[d, part], c_recv.at[slot, part], c_ssem.at[d, i], c_rsem.at[slot, i], {"dp": me + toward})

        def own_sum(d, i):
            part = pl.ds(pl.multiple_of(i * piece, piece), piece)
            partial(d, i).wait_recv()
            acc[...] = dx_tile(d, row * half + i * piece, piece) + p_recv[d, part, :].astype(jnp.float32)

        def add_incoming(slot, i):
            part = pl.ds(pl.multiple_of(i * piece, piece), piece)
            remote(
                c_recv.at[slot, part], c_recv.at[slot, part], c_ssem.at[0, i], c_rsem.at[slot, i], {"row": partner}
            ).wait_recv()
            acc[...] = acc[...] + c_recv[slot, part, :].astype(jnp.float32)

        def pass_on(d, toward):
            def body(i, carry):
                part = pl.ds(pl.multiple_of(i * piece, piece), piece)
                own_sum(d, i)
                has_incoming = me > 0 if toward > 0 else me < n_dp - 1

                @pl.when(has_incoming)
                def _():
                    add_incoming(d, i)

                c_send[d, part, :] = acc[...].astype(jnp.bfloat16)
                if toward > 0:
                    chain(d, d, i, 1).start()
                else:
                    last = (n_dp - 1 - (me - 1 - d)) // (n_dp - 1)
                    chain(d, d + last * (n_dp - d), i, -1).start()
                return carry

            lax.fori_loop(0, pieces, body, 0)

        def pass_up(d):
            @pl.when(me < d)
            def _():
                pass_on(d, 1)

        def pass_down(d):
            @pl.when(me > d)
            def _():
                pass_on(d, -1)

        def take_a(k):
            @pl.when(me - k >= 0)
            def _():
                d = me - k
                arrived_a(d, row)

                @pl.when(me < n_dp - 1)
                def _():
                    send_a(d, 1).start()

                swap_a(d).start()

            @pl.when(me + k < n_dp)
            def _():
                d = me + k
                arrived_a(d, row)

                @pl.when(me > 0)
                def _():
                    send_a(d, -1).start()

                swap_a(d).start()

        def products_at(k):
            for sign in (-1, 1):
                inside = me - k >= 0 if sign < 0 else me + k < n_dp

                @pl.when(inside)
                def _():
                    d = me + sign * k
                    arrived_a(d, partner)
                    add_products(d)

        mid = n_dp // 2
        order = [(mid + j, mid - 1 - j) for j in range(n_dp - mid)]
        order += [(d, n_dp - 1 - d) for d in range(1, mid)]
        for k in range(1, n_dp):
            take_a(k)
            if k > 2:
                products_at(k - 1)
            up, down = order[k - 1]
            pass_up(up)
            pass_down(down)
            if k == 2:
                products_at(1)
        products_at(n_dp - 1)

        def store(k):
            return pltpu.make_async_copy(
                prod.at[pl.ds(k * block, block)], weight_grad.at[0, pl.ds(k * block, block)], out_sem.at[k]
            )

        load_w(0).start()
        load_w(1).start()
        for k in range(n_block):
            load_w(k).wait()
            ratio, _ = ratio_of(k)
            clipped = jnp.clip(ratio, -8.0, 7.0)
            inside = (ratio >= -8.0) & (ratio <= 7.0)
            factor = jnp.where(inside, jnp.floor(clipped + 0.5) - ratio, clipped)
            rows = pl.ds(k * block, block)
            values = prod[rows, :]
            share = values * factor
            lanes = share[:, 0:128]
            for j in range(1, width // 128):
                lanes = lanes + share[:, j * 128:(j + 1) * 128]
            sg_buf[0, :, rows] = jnp.sum(jnp.transpose(lanes), axis=0, keepdims=True) * factor_scale
            prod[rows, :] = jnp.where(inside, values, 0.0)
            store(k).start()
            if k + 2 < n_block:
                load_w(k + 2).start()

        def swap_steps(b):
            return remote(sg_buf.at[b], sg_in.at[b], sg_ssem.at[b], sg_rsem.at[b], {"col": flipped(col, bits[b])})

        for b in range(len(bits)):
            swap_steps(b).start()
            swap_steps(b).wait_recv()
            sg_buf[b + 1] = sg_buf[b] + sg_in[b]
        step_grad[...] = sg_buf[len(bits)]

        def finish(i, carry):
            part = pl.ds(pl.multiple_of(i * piece, piece), piece)
            own_sum(me, i)

            @pl.when(me > 0)
            def _():
                add_incoming(me, i)

            @pl.when(me < n_dp - 1)
            def _():
                add_incoming(n_dp, i)

            input_grad[part, :] = acc[...].astype(jnp.bfloat16)
            return carry

        lax.fori_loop(0, pieces, finish, 0)

        each_target(lambda t: send_g(t).wait_send())
        for s in range(n_dp - 1):
            d = nth(s)
            hypercube(d, lambda *a: None, lambda *a: forward_g(*a).wait_send())
            swap_a(d).wait_send()

        @pl.when(me < n_dp - 1)
        def _():
            send_a(None, 1).wait_send()

        @pl.when(me > 0)
        def _():
            send_a(None, -1).wait_send()

        for k in range(1, n_dp):
            @pl.when((me - k >= 0) & (me < n_dp - 1))
            def _():
                send_a(me - k, 1).wait_send()

            @pl.when((me + k < n_dp) & (me > 0))
            def _():
                send_a(me + k, -1).wait_send()

        def drain(d, carry):
            def each(i, inner):
                partial(d, i).wait_send()

                @pl.when(me != d)
                def _():
                    part = pl.ds(pl.multiple_of(i * piece, piece), piece)
                    remote(
                        c_send.at[d, part], c_send.at[d, part], c_ssem.at[d, i], c_rsem.at[d, i], {"row": partner}
                    ).wait_send()

                return inner

            return lax.fori_loop(0, pieces, each, carry)

        lax.fori_loop(0, n_dp, drain, 0)
        for b in range(len(bits)):
            swap_steps(b).wait_send()
        for k in range(n_block):
            store(k).wait()

    scratch = [
        pltpu.VMEM((n_dp, tokens, own), jnp.bfloat16),
        pltpu.VMEM((n_dp, tokens, width), jnp.bfloat16),
        pltpu.VMEM((own, width), jnp.bfloat16),
        pltpu.VMEM((own, width), jnp.float32),
        pltpu.VMEM((n_dp, half, width), jnp.bfloat16),
        pltpu.VMEM((n_dp, half, width), jnp.bfloat16),
        pltpu.VMEM((n_dp, half, width), jnp.bfloat16),
        pltpu.VMEM((n_dp + 1, half, width), jnp.bfloat16),
        pltpu.VMEM((2, block, width), jnp.float32),
        pltpu.VMEM((own, 128), jnp.float32),
        pltpu.VMEM((piece, width), jnp.float32),
        pltpu.VMEM((len(bits) + 1, 1, own), jnp.float32),
        pltpu.VMEM((len(bits), 1, own), jnp.float32),
        pltpu.SemaphoreType.DMA((2,)),
        pltpu.SemaphoreType.DMA((2,)),
        pltpu.SemaphoreType.DMA((own // block,)),
        pltpu.SemaphoreType.DMA((n_dp,)),
        pltpu.SemaphoreType.DMA((n_dp, n_col)),
        pltpu.SemaphoreType.DMA((n_dp, n_col - 1)),
        pltpu.SemaphoreType.DMA((n_dp, 2)),
        pltpu.SemaphoreType.DMA((n_dp,)),
        pltpu.SemaphoreType.DMA((n_dp, n_row)),
        pltpu.SemaphoreType.DMA((n_dp, pieces)),
        pltpu.SemaphoreType.DMA((n_dp, pieces)),
        pltpu.SemaphoreType.DMA((n_dp, pieces)),
        pltpu.SemaphoreType.DMA((n_dp + 1, pieces)),
        pltpu.SemaphoreType.DMA((len(bits),)),
        pltpu.SemaphoreType.DMA((len(bits),)),
    ]
    anywhere = pl.BlockSpec(memory_space=pl.ANY)
    inside = pl.BlockSpec(memory_space=pltpu.VMEM)
    return pl.pallas_call(
        kernel,
        out_shape=(
            jax.ShapeDtypeStruct((half, width), jnp.bfloat16),
            jax.ShapeDtypeStruct((1, own, width), jnp.float32),
            jax.ShapeDtypeStruct((1, own), jnp.float32),
        ),
        in_specs=[anywhere, anywhere, anywhere, inside],
        out_specs=(inside, anywhere, inside),
        scratch_shapes=scratch,
        compiler_params=pltpu.CompilerParams(collective_id=0, has_side_effects=True, vmem_limit_bytes=67043328),
        name="backward",
    )


def fits(n_dp, n_row, n_col, activations, weight):
    tokens, width = activations.shape
    own = weight.shape[1]
    return (
        n_dp % 2 == 0 and n_row == 2 and n_col > 1 and n_col & (n_col - 1) == 0
        and own % 256 == 0 and width % 128 == 0 and tokens % (128 * n_row) == 0 and tokens % (16 * n_col) == 0
        and n_dp * tokens * (own + width) <= 12 * 2**20
    )


def solution(mesh):
    n_dp, n_row, n_col = mesh.shape["dp"], mesh.shape["row"], mesh.shape["col"]
    in_specs = (P("dp", "col"), P("dp", "row"), P("row", "dp", "col"), P("row", None))
    out_specs = (P(("dp", "row"), "col"), P("row", "dp", "col"), P("row", "dp"))
    general = make_shards(n_dp, n_row, n_col)

    def shards(activations, out_grad, weight, step_size):
        if not fits(n_dp, n_row, n_col, activations, weight):
            return general(activations, out_grad, weight, step_size)
        tokens, width = activations.shape
        call = make_kernel(n_dp, n_row, n_col, tokens, weight.shape[1], width)
        return call(activations, out_grad, weight, step_size)

    return jax.shard_map(shards, mesh=mesh, in_specs=in_specs, out_specs=out_specs, check_vma=False)
```

```python
import jax
import jax.numpy as jnp
from jax import lax
from jax.experimental.layout import Layout, with_layout_constraint
from jax.experimental import pallas as pl
from jax.experimental.pallas import tpu as pltpu
from jax.sharding import PartitionSpec as P

D = 4096


def quantize(latent, scales):
    ratio = latent / scales[:, None]
    clipped = jnp.clip(ratio, -8.0, 7.0)
    levels = jnp.floor(clipped + 0.5)
    inside = jnp.where((ratio >= -8.0) & (ratio <= 7.0), 1.0, 0.0).astype(jnp.float32)
    factor = jnp.where(inside > 0.5, levels - ratio, clipped)
    quantized = (levels * scales[:, None]).astype(jnp.bfloat16)
    return (quantized, inside, factor)


def shift(block, axis, count, by):
    return lax.ppermute(block, axis, [(i, (i + by) % count) for i in range(count)])


def swap(block, axis, count, bit):
    return lax.ppermute(block, axis, [(i, i ^ bit) for i in range(count)])


def gather_rows(block, axis, count):
    position = lax.axis_index(axis)
    bit = 1
    bits = []
    while bit < count:
        bits.append(bit)
        bit *= 2
    pieces = {0: block}
    for bit in reversed(bits):
        held = dict(pieces)
        for key in held:
            pieces[key ^ bit] = swap(held[key], axis, count, bit)
    parts = [pieces[key] for key in range(count)]
    for bit in bits:
        flag = (position & bit) != 0
        parts = [
            jnp.where(flag, parts[key ^ bit], parts[key]) for key in range(count)
        ]
    return jnp.concatenate(parts, axis=0)


def make_shards(n_dp, n_row, n_col):
    def shards(activations, out_grad, weight, step_size):
        own_count = weight.shape[1]
        tokens = out_grad.shape[0]
        dp = lax.axis_index("dp")
        row = lax.axis_index("row")
        col = lax.axis_index("col")
        scales = step_size[0]
        own_scales = lax.dynamic_slice_in_dim(scales, dp * own_count, own_count, 0)
        grad_factor = 1.0 / (7.0 * D) ** 0.5

        share = tokens // n_col
        half = tokens // n_row
        mine = lax.dynamic_slice_in_dim(out_grad, col * share, share, 0)
        ring = lax.dynamic_slice_in_dim(activations, row * half, half, 0)
        grads, acts = [], []
        for k in range(1, n_dp):
            target = (dp + k) % n_dp
            chunk = lax.dynamic_slice_in_dim(mine, target * own_count, own_count, 1)
            grads.append(shift(chunk, "dp", n_dp, k))
            ring = shift(ring, "dp", n_dp, 1)
            acts.append(ring)

        quantized, _, _ = quantize(weight[0], own_scales)
        own_grad = lax.dynamic_slice_in_dim(out_grad, dp * own_count, own_count, 1)

        def reduced(grad):
            size = tokens
            bit = n_row // 2
            if bit == 0:
                return jnp.dot(grad, quantized, preferred_element_type=jnp.float32)
            size //= 2
            upper = ((row // bit) % 2).astype(jnp.int32)
            sent = lax.dynamic_slice_in_dim(grad, (1 - upper) * size, size, 0)
            kept = lax.dynamic_slice_in_dim(grad, upper * size, size, 0)
            out = jnp.dot(sent, quantized, preferred_element_type=jnp.float32).astype(jnp.bfloat16)
            came = swap(out, "row", n_row, bit)
            total = jnp.dot(kept, quantized, preferred_element_type=jnp.float32) + came.astype(jnp.float32)
            bit //= 2
            while bit:
                size //= 2
                upper = (row // bit) % 2 == 1
                low, high = total[:size], total[size:]
                came = swap(jnp.where(upper, low, high).astype(jnp.bfloat16), "row", n_row, bit)
                total = jnp.where(upper, high, low) + came.astype(jnp.float32)
                bit //= 2
            return total

        products = lax.dot_general(
            own_grad, activations, (((0,), (0,)), ((), ())), preferred_element_type=jnp.float32
        )
        own_total = reduced(own_grad)
        if grads:
            grads[0], quantized, products = lax.optimization_barrier((grads[0], quantized, products))
        running = None
        for k in range(1, n_dp):
            grad = gather_rows(grads[k - 1], "col", n_col)
            total = reduced(grad)
            if running is not None:
                total = total + running.astype(jnp.float32)
            leaving, grad = lax.optimization_barrier((total.astype(jnp.bfloat16), grad))
            running = shift(leaving, "dp", n_dp, 1)
            act = gather_rows(acts[k - 1], "row", n_row)
            products = products + lax.dot_general(
                grad, act, (((0,), (0,)), ((), ())), preferred_element_type=jnp.float32
            )
        if running is not None:
            own_total = own_total + running.astype(jnp.float32)
        products, latent = lax.optimization_barrier((products, weight[0]))
        products = with_layout_constraint(products, Layout((0, 1)))
        _, inside, factor = quantize(latent, own_scales)
        input_grad = own_total.astype(jnp.bfloat16)
        step_rows = lax.psum(jnp.sum(products * factor, axis=1) * grad_factor, "col")
        weight_grad = (products * inside)[None]
        return (input_grad, weight_grad, step_rows[None])

    return shards


MESH = pl.DeviceIdType.MESH


def flipped(position, bit):
    return position + bit * (1 - 2 * lax.rem(position // bit, 2))


def make_kernel(n_dp, n_row, n_col, tokens, own, width):
    quarter = tokens // n_col
    half = tokens // n_row
    piece = 128
    pieces = half // piece
    block = 256
    halves = 2
    g_rows = quarter // halves
    a_rows = half // halves
    factor_scale = 1.0 / (7.0 * width * n_col) ** 0.5
    bits = []
    bit = n_col // 2
    while bit:
        bits.append(bit)
        bit //= 2

    def kernel(act, out_grad, weight, steps, input_grad, weight_grad, step_grad,
               g_buf, a_buf, q_buf, f_buf, p_send, p_recv, c_send, c_recv, w_buf, s_buf, acc, sg_buf, sg_in,
               load_sem, w_sem, gz_send, g_recv, gx_send, az_send, ay_send, a_recv,
               p_ssem, p_rsem, c_ssem, c_rsem, sg_ssem, sg_rsem):
        prod = weight_grad.at[0]
        me = lax.axis_index("dp")
        row = lax.axis_index("row")
        col = lax.axis_index("col")
        partner = 1 - row

        def remote(src, dst, send, recv, where):
            return pltpu.make_async_remote_copy(
                src_ref=src, dst_ref=dst, send_sem=send, recv_sem=recv, device_id=where, device_id_type=MESH
            )

        def rows_of(index, size):
            return pl.ds(pl.multiple_of(index * size, size), size)

        barrier = pltpu.get_barrier_semaphore()
        for k in range(1, n_dp):
            pl.semaphore_signal(barrier, inc=1, device_id={"dp": lax.rem(me + k, n_dp)}, device_id_type=MESH)
        pl.semaphore_signal(barrier, inc=1, device_id={"row": partner}, device_id_type=MESH)
        columns_by = [col]
        for bit in reversed(bits):
            columns_by += [flipped(which, bit) for which in columns_by]
        for which in columns_by[1:]:
            pl.semaphore_signal(barrier, inc=1, device_id={"col": which}, device_id_type=MESH)

        own_columns = pl.ds(pl.multiple_of(me * own, 128), own)
        load_g = pltpu.make_async_copy(out_grad.at[:, own_columns], g_buf.at[me], load_sem.at[0])
        load_a = pltpu.make_async_copy(act, a_buf.at[me], load_sem.at[1])

        def load_w(k):
            return pltpu.make_async_copy(weight.at[0, pl.ds(k * block, block)], w_buf.at[k % 2], w_sem.at[k % 2])

        load_w(0).start()
        load_w(1).start()
        load_g.start()
        load_a.start()
        pl.semaphore_wait(barrier, n_dp - 1 + 1 + n_col - 1)

        def g_span(which, h):
            return pl.ds(pl.multiple_of(which * quarter + h * g_rows, g_rows), g_rows)

        def send_g(target, h):
            columns = pl.ds(pl.multiple_of(target * own, 128), own)
            return remote(
                out_grad.at[g_span(col, h), columns], g_buf.at[me, g_span(col, h)],
                gz_send.at[target, h], g_recv.at[me, col, h], {"dp": target},
            )

        upper = me // (n_dp // 2)

        def at(position):
            return position + upper * (n_dp - 1 - 2 * position)

        toward = 1 - 2 * upper
        place = at(me)
        spot = [at(position) for position in range(n_dp)]
        started = ([], [])

        def go(role, make):
            make().start()
            started[role].append(make)

        def give_g(role, target):
            for h in range(halves):
                go(role, lambda h=h: send_g(target, h))

        @pl.when(place == 0)
        def _():
            give_g(0, spot[1])

        @pl.when(place == 1)
        def _():
            give_g(1, spot[2])
            give_g(1, spot[0])

        def a_span(which, h):
            return pl.ds(pl.multiple_of(which * half + h * a_rows, a_rows), a_rows)

        def send_a(source, inward, h, which, slot, own=False):
            span = a_span(which, h)
            return remote(
                act.at[span] if own else a_buf.at[source, span], a_buf.at[source, span],
                az_send.at[slot, inward, h], a_recv.at[source, which, h], {"dp": me + (2 * inward - 1) * toward},
            )

        def swap_a(source, h):
            span = a_span(row, h)
            return remote(
                a_buf.at[source, span], a_buf.at[source, span], ay_send.at[source, h], a_recv.at[source, row, h],
                {"row": partner},
            )

        def arrived_a(source, which, h):
            span = a_span(which, h)
            remote(
                a_buf.at[source, span], a_buf.at[source, span], ay_send.at[source, h], a_recv.at[source, which, h],
                {"row": partner},
            ).wait_recv()

        def give_a(role, inward, other=False):
            which, slot = (partner, n_dp) if other else (row, me)
            for h in range(halves):
                go(role, lambda h=h: send_a(me, inward, h, which, slot, own=True))

        for k in range(own // 128):
            values = steps[0:1, pl.ds(pl.multiple_of(me * own + k * 128, 128), 128)]
            s_buf[pl.ds(k * 128, 128), :] = jnp.transpose(jnp.broadcast_to(values, (128, 128)))

        n_block = own // block

        for k in range(n_block):
            load_w(k).wait()
            s = jnp.concatenate([s_buf[pl.ds(k * block, block), :]] * (width // 128), axis=1)
            ratio = w_buf[k % 2] / s
            clipped = jnp.clip(ratio, -8.0, 7.0)
            levels = jnp.floor(clipped + 0.5)
            q_buf[pl.ds(k * block, block), :] = (levels * s).astype(jnp.bfloat16)
            f_buf[pl.ds(k * block, block), :] = jnp.where(clipped == ratio, levels - ratio, clipped).astype(jnp.bfloat16)
            if k + 2 < n_block:
                load_w(k + 2).start()
        load_g.wait()

        def dx_tile(d, start, size):
            return jnp.dot(
                g_buf[d, pl.ds(pl.multiple_of(start, size), size), :], q_buf[...], preferred_element_type=jnp.float32
            )

        def partial(d, i):
            part = pl.ds(pl.multiple_of(i * piece, piece), piece)
            return remote(p_send.at[d, part], p_recv.at[d, part], p_ssem.at[d, i], p_rsem.at[d, i], {"row": partner})

        def send_partials(d):
            def body(i, carry):
                p_send[d, pl.ds(pl.multiple_of(i * piece, piece), piece), :] = dx_tile(
                    d, partner * half + i * piece, piece
                ).astype(jnp.bfloat16)
                partial(d, i).start()
                return carry

            lax.fori_loop(0, pieces, body, 0)

        def add_products(d, first=False, last=False):
            def body(k, carry):
                rows = pl.ds(pl.multiple_of(k * block, block), block)
                new = lax.dot_general(
                    g_buf[d, :, rows], a_buf[d], (((0,), (0,)), ((), ())), preferred_element_type=jnp.float32
                )
                if not first:
                    new = new + prod[rows, :]
                if last:
                    factor = f_buf[rows, :].astype(jnp.float32)
                    prod[rows, :] = jnp.where(jnp.abs(factor) < 1.0, new, 0.0)
                    share = new * factor
                    lanes = share[:, 0:128]
                    for j in range(1, width // 128):
                        lanes = lanes + share[:, j * 128:(j + 1) * 128]
                    sg_buf[:, rows] = jnp.sum(jnp.transpose(lanes), axis=0, keepdims=True) * factor_scale
                else:
                    prod[rows, :] = new
                return carry

            lax.fori_loop(0, n_block, body, 0)

        send_partials(me)
        load_a.wait()
        add_products(me, first=True)

        def forward_g(d, differs, bit, slot, h):
            span = g_span(columns_by[differs], h)
            return remote(
                g_buf.at[d, span], g_buf.at[d, span], gx_send.at[d, slot, h], g_recv.at[d, columns_by[differs], h],
                {"col": columns_by[bit]},
            )

        def arrived_g(d, differs, h):
            forward_g(d, differs, bits[0], 0, h).wait_recv()

        def first_g(role, d, then=None):
            for h in range(halves):
                arrived_g(d, 0, h)
                for slot, bit in enumerate(bits):
                    go(role, lambda bit=bit, slot=slot, h=h: forward_g(d, 0, bit, slot, h))
                if h == 0 and then is not None:
                    then()

        def rest_g(role, d):
            slot, held = len(bits), [0]
            for b, bit in enumerate(bits):
                come = [differs ^ bit for differs in held]
                for differs in come:
                    later = bits[b + 1:]
                    for h in range(halves):
                        arrived_g(d, differs, h)
                        for j, over in enumerate(later):
                            go(role, lambda differs=differs, over=over, slot=slot + j, h=h: forward_g(d, differs, over, slot, h))
                    slot += len(later)
                held += come
            send_partials(d)

        def chain(d, slot, i, step):
            part = pl.ds(pl.multiple_of(i * piece, piece), piece)
            return remote(c_send.at[d, part], c_recv.at[slot, part], c_ssem.at[d, i], c_rsem.at[slot, i], {"dp": me + step})

        def own_sum(d, i):
            part = pl.ds(pl.multiple_of(i * piece, piece), piece)
            partial(d, i).wait_recv()
            acc[...] = dx_tile(d, row * half + i * piece, piece) + p_recv[d, part, :].astype(jnp.float32)

        def add_incoming(slot, i):
            part = pl.ds(pl.multiple_of(i * piece, piece), piece)
            remote(
                c_recv.at[slot, part], c_recv.at[slot, part], c_ssem.at[0, i], c_rsem.at[slot, i], {"row": partner}
            ).wait_recv()
            acc[...] = acc[...] + c_recv[slot, part, :].astype(jnp.float32)

        def pass_on(d, inward, first=False, last=False):
            step = toward * (2 * inward - 1)
            slot = d + (1 - step) // 2 * (n_dp - d) if last else d

            def body(i, carry):
                part = pl.ds(pl.multiple_of(i * piece, piece), piece)
                own_sum(d, i)
                if not first:
                    add_incoming(d, i)
                c_send[d, part, :] = acc[...].astype(jnp.bfloat16)
                chain(d, slot, i, step).start()
                return carry

            lax.fori_loop(0, pieces, body, 0)

        def take_a(role, d, onward=()):
            for h in range(halves):
                arrived_a(d, row, h)
                for inward in onward:
                    go(role, lambda inward=inward, h=h: send_a(d, inward, h, row, d))
                go(role, lambda h=h: swap_a(d, h))

        def products_of(d, both=False, last=False):
            for which in (row, partner) if both else (partner,):
                for h in range(halves):
                    arrived_a(d, which, h)
            add_products(d, last=last)

        def finish():
            def body(i, carry):
                part = pl.ds(pl.multiple_of(i * piece, piece), piece)
                own_sum(me, i)

                @pl.when(me > 0)
                def _():
                    add_incoming(me, i)

                @pl.when(me < n_dp - 1)
                def _():
                    add_incoming(n_dp, i)

                input_grad[part, :] = acc[...].astype(jnp.bfloat16)
                return carry

            lax.fori_loop(0, pieces, body, 0)

        def swap_steps(differs):
            return remote(
                sg_buf, sg_in.at[differs - 1], sg_ssem.at[differs - 1], sg_rsem.at[differs - 1],
                {"col": columns_by[differs]},
            )

        def give_steps(role):
            for differs in range(1, n_col):
                go(role, lambda differs=differs: swap_steps(differs))

        @pl.when(place == 0)
        def _():
            r = 0
            first_g(r, spot[1], lambda: give_g(r, spot[2]))
            rest_g(r, spot[1])
            give_a(r, 1)
            first_g(r, spot[2], lambda: give_g(r, spot[3]))
            rest_g(r, spot[2])
            first_g(r, spot[3])
            pass_on(spot[1], 1, first=True, last=True)
            rest_g(r, spot[3])
            pass_on(spot[2], 1, first=True)
            pass_on(spot[3], 1, first=True)
            take_a(r, spot[2])
            products_of(spot[1], both=True)
            take_a(r, spot[3])
            products_of(spot[2])
            products_of(spot[3], last=True)
            give_steps(r)
            finish()

        @pl.when(place == 1)
        def _():
            r = 1
            first_g(r, spot[0], lambda: give_a(r, 0))
            first_g(r, spot[2])
            give_g(r, spot[3])
            rest_g(r, spot[0])
            first_g(r, spot[3])
            rest_g(r, spot[2])
            give_a(r, 1)
            rest_g(r, spot[3])
            give_a(r, 0, other=True)
            take_a(r, spot[0], (1,))
            take_a(r, spot[2], (0,))
            take_a(r, spot[3], (0,))
            pass_on(spot[2], 1, last=True)
            products_of(spot[0])
            pass_on(spot[3], 1)
            finish()
            products_of(spot[2])
            pass_on(spot[0], 0, last=True)
            products_of(spot[3], last=True)
            give_steps(r)

        for differs in range(1, n_col):
            swap_steps(differs).wait_recv()
        total = sg_buf[...]
        for differs in range(1, n_col):
            total = total + sg_in[differs - 1]
        step_grad[...] = total

        for role in range(2):
            @pl.when(place == role)
            def _():
                for make in started[role]:
                    make().wait_send()

        def drain(d, carry):
            def each(i, inner):
                partial(d, i).wait_send()

                @pl.when(me != d)
                def _():
                    part = pl.ds(pl.multiple_of(i * piece, piece), piece)
                    remote(
                        c_send.at[d, part], c_send.at[d, part], c_ssem.at[d, i], c_rsem.at[d, i], {"row": partner}
                    ).wait_send()

                return inner

            return lax.fori_loop(0, pieces, each, carry)

        lax.fori_loop(0, n_dp, drain, 0)
    scratch = [
        pltpu.VMEM((n_dp, tokens, own), jnp.bfloat16),
        pltpu.VMEM((n_dp, tokens, width), jnp.bfloat16),
        pltpu.VMEM((own, width), jnp.bfloat16),
        pltpu.VMEM((own, width), jnp.bfloat16),
        pltpu.VMEM((n_dp, half, width), jnp.bfloat16),
        pltpu.VMEM((n_dp, half, width), jnp.bfloat16),
        pltpu.VMEM((n_dp, half, width), jnp.bfloat16),
        pltpu.VMEM((n_dp + 1, half, width), jnp.bfloat16),
        pltpu.VMEM((2, block, width), jnp.float32),
        pltpu.VMEM((own, 128), jnp.float32),
        pltpu.VMEM((piece, width), jnp.float32),
        pltpu.VMEM((1, own), jnp.float32),
        pltpu.VMEM((n_col - 1, 1, own), jnp.float32),
        pltpu.SemaphoreType.DMA((2,)),
        pltpu.SemaphoreType.DMA((2,)),
        pltpu.SemaphoreType.DMA((n_dp, halves)),
        pltpu.SemaphoreType.DMA((n_dp, n_col, halves)),
        pltpu.SemaphoreType.DMA((n_dp, n_col - 1, halves)),
        pltpu.SemaphoreType.DMA((n_dp + 1, 2, halves)),
        pltpu.SemaphoreType.DMA((n_dp, halves)),
        pltpu.SemaphoreType.DMA((n_dp, n_row, halves)),
        pltpu.SemaphoreType.DMA((n_dp, pieces)),
        pltpu.SemaphoreType.DMA((n_dp, pieces)),
        pltpu.SemaphoreType.DMA((n_dp, pieces)),
        pltpu.SemaphoreType.DMA((n_dp + 1, pieces)),
        pltpu.SemaphoreType.DMA((n_col - 1,)),
        pltpu.SemaphoreType.DMA((n_col - 1,)),
    ]
    anywhere = pl.BlockSpec(memory_space=pl.ANY)
    inside = pl.BlockSpec(memory_space=pltpu.VMEM)
    return pl.pallas_call(
        kernel,
        out_shape=(
            pltpu.VMEM((half, width), jnp.bfloat16),
            pltpu.VMEM((1, own, width), jnp.float32),
            pltpu.VMEM((1, own), jnp.float32),
        ),
        in_specs=[anywhere, anywhere, anywhere, inside],
        out_specs=(inside, inside, inside),
        scratch_shapes=scratch,
        compiler_params=pltpu.CompilerParams(collective_id=0, has_side_effects=True, vmem_limit_bytes=54 * 2**20),
        name="backward",
    )


def fits(n_dp, n_row, n_col, activations, weight):
    tokens, width = activations.shape
    own = weight.shape[1]
    return (
        n_dp == 4 and n_row == 2 and n_col > 1 and n_col & (n_col - 1) == 0
        and own % 256 == 0 and width % 128 == 0 and tokens % (128 * n_row) == 0 and tokens % (32 * n_col) == 0
        and n_dp * tokens * (own + width) <= 12 * 2**20
    )


def solution(mesh):
    n_dp, n_row, n_col = mesh.shape["dp"], mesh.shape["row"], mesh.shape["col"]
    in_specs = (P("dp", "col"), P("dp", "row"), P("row", "dp", "col"), P("row", None))
    out_specs = (P(("dp", "row"), "col"), P("row", "dp", "col"), P("row", "dp"))
    general = make_shards(n_dp, n_row, n_col)

    def shards(activations, out_grad, weight, step_size):
        if not fits(n_dp, n_row, n_col, activations, weight):
            return general(activations, out_grad, weight, step_size)
        tokens, width = activations.shape
        call = make_kernel(n_dp, n_row, n_col, tokens, weight.shape[1], width)
        return call(activations, out_grad, weight, step_size)

    return jax.shard_map(shards, mesh=mesh, in_specs=in_specs, out_specs=out_specs, check_vma=False)
```

```python
import jax
import jax.numpy as jnp
from jax import lax
from jax.experimental.layout import Layout, with_layout_constraint
from jax.experimental import pallas as pl
from jax.experimental.pallas import tpu as pltpu
from jax.sharding import PartitionSpec as P

D = 4096


def quantize(latent, scales):
    ratio = latent / scales[:, None]
    clipped = jnp.clip(ratio, -8.0, 7.0)
    levels = jnp.floor(clipped + 0.5)
    inside = jnp.where((ratio >= -8.0) & (ratio <= 7.0), 1.0, 0.0).astype(jnp.float32)
    factor = jnp.where(inside > 0.5, levels - ratio, clipped)
    quantized = (levels * scales[:, None]).astype(jnp.bfloat16)
    return (quantized, inside, factor)


def shift(block, axis, count, by):
    return lax.ppermute(block, axis, [(i, (i + by) % count) for i in range(count)])


def swap(block, axis, count, bit):
    return lax.ppermute(block, axis, [(i, i ^ bit) for i in range(count)])


def gather_rows(block, axis, count):
    position = lax.axis_index(axis)
    bit = 1
    bits = []
    while bit < count:
        bits.append(bit)
        bit *= 2
    pieces = {0: block}
    for bit in reversed(bits):
        held = dict(pieces)
        for key in held:
            pieces[key ^ bit] = swap(held[key], axis, count, bit)
    parts = [pieces[key] for key in range(count)]
    for bit in bits:
        flag = (position & bit) != 0
        parts = [
            jnp.where(flag, parts[key ^ bit], parts[key]) for key in range(count)
        ]
    return jnp.concatenate(parts, axis=0)


def make_shards(n_dp, n_row, n_col):
    def shards(activations, out_grad, weight, step_size):
        own_count = weight.shape[1]
        tokens = out_grad.shape[0]
        dp = lax.axis_index("dp")
        row = lax.axis_index("row")
        col = lax.axis_index("col")
        scales = step_size[0]
        own_scales = lax.dynamic_slice_in_dim(scales, dp * own_count, own_count, 0)
        grad_factor = 1.0 / (7.0 * D) ** 0.5

        share = tokens // n_col
        half = tokens // n_row
        mine = lax.dynamic_slice_in_dim(out_grad, col * share, share, 0)
        ring = lax.dynamic_slice_in_dim(activations, row * half, half, 0)
        grads, acts = [], []
        for k in range(1, n_dp):
            target = (dp + k) % n_dp
            chunk = lax.dynamic_slice_in_dim(mine, target * own_count, own_count, 1)
            grads.append(shift(chunk, "dp", n_dp, k))
            ring = shift(ring, "dp", n_dp, 1)
            acts.append(ring)

        quantized, _, _ = quantize(weight[0], own_scales)
        own_grad = lax.dynamic_slice_in_dim(out_grad, dp * own_count, own_count, 1)

        def reduced(grad):
            size = tokens
            bit = n_row // 2
            if bit == 0:
                return jnp.dot(grad, quantized, preferred_element_type=jnp.float32)
            size //= 2
            upper = ((row // bit) % 2).astype(jnp.int32)
            sent = lax.dynamic_slice_in_dim(grad, (1 - upper) * size, size, 0)
            kept = lax.dynamic_slice_in_dim(grad, upper * size, size, 0)
            out = jnp.dot(sent, quantized, preferred_element_type=jnp.float32).astype(jnp.bfloat16)
            came = swap(out, "row", n_row, bit)
            total = jnp.dot(kept, quantized, preferred_element_type=jnp.float32) + came.astype(jnp.float32)
            bit //= 2
            while bit:
                size //= 2
                upper = (row // bit) % 2 == 1
                low, high = total[:size], total[size:]
                came = swap(jnp.where(upper, low, high).astype(jnp.bfloat16), "row", n_row, bit)
                total = jnp.where(upper, high, low) + came.astype(jnp.float32)
                bit //= 2
            return total

        products = lax.dot_general(
            own_grad, activations, (((0,), (0,)), ((), ())), preferred_element_type=jnp.float32
        )
        own_total = reduced(own_grad)
        if grads:
            grads[0], quantized, products = lax.optimization_barrier((grads[0], quantized, products))
        running = None
        for k in range(1, n_dp):
            grad = gather_rows(grads[k - 1], "col", n_col)
            total = reduced(grad)
            if running is not None:
                total = total + running.astype(jnp.float32)
            leaving, grad = lax.optimization_barrier((total.astype(jnp.bfloat16), grad))
            running = shift(leaving, "dp", n_dp, 1)
            act = gather_rows(acts[k - 1], "row", n_row)
            products = products + lax.dot_general(
                grad, act, (((0,), (0,)), ((), ())), preferred_element_type=jnp.float32
            )
        if running is not None:
            own_total = own_total + running.astype(jnp.float32)
        products, latent = lax.optimization_barrier((products, weight[0]))
        products = with_layout_constraint(products, Layout((0, 1)))
        _, inside, factor = quantize(latent, own_scales)
        input_grad = own_total.astype(jnp.bfloat16)
        step_rows = lax.psum(jnp.sum(products * factor, axis=1) * grad_factor, "col")
        weight_grad = (products * inside)[None]
        return (input_grad, weight_grad, step_rows[None])

    return shards


MESH = pl.DeviceIdType.MESH


def flipped(position, bit):
    return position + bit * (1 - 2 * lax.rem(position // bit, 2))


def make_kernel(n_dp, n_row, n_col, tokens, own, width):
    quarter = tokens // n_col
    half = tokens // n_row
    piece = 128
    pieces = half // piece
    block = 256
    halves = 2
    g_rows = quarter // halves
    a_rows = half // halves
    factor_scale = 1.0 / (7.0 * width * n_col) ** 0.5
    bits = []
    bit = n_col // 2
    while bit:
        bits.append(bit)
        bit //= 2

    def kernel(act, out_grad, weight, steps, input_grad, weight_grad, step_grad,
               g_buf, a_buf, q_buf, f_buf, p_send, p_recv, c_send, c_recv, w_buf, s_buf, acc, sg_buf, sg_in,
               load_sem, w_sem, gz_send, g_recv, gx_send, az_send, ay_send, a_recv,
               p_ssem, p_rsem, c_ssem, c_rsem, sg_ssem, sg_rsem):
        prod = weight_grad.at[0]
        me = lax.axis_index("dp")
        row = lax.axis_index("row")
        col = lax.axis_index("col")
        partner = 1 - row

        def remote(src, dst, send, recv, where):
            return pltpu.make_async_remote_copy(
                src_ref=src, dst_ref=dst, send_sem=send, recv_sem=recv, device_id=where, device_id_type=MESH
            )

        def rows_of(index, size):
            return pl.ds(pl.multiple_of(index * size, size), size)

        barrier = pltpu.get_barrier_semaphore()
        for k in range(1, n_dp):
            pl.semaphore_signal(barrier, inc=1, device_id={"dp": lax.rem(me + k, n_dp)}, device_id_type=MESH)
        pl.semaphore_signal(barrier, inc=1, device_id={"row": partner}, device_id_type=MESH)
        columns_by = [col]
        for bit in reversed(bits):
            columns_by += [flipped(which, bit) for which in columns_by]
        for which in columns_by[1:]:
            pl.semaphore_signal(barrier, inc=1, device_id={"col": which}, device_id_type=MESH)

        own_columns = pl.ds(pl.multiple_of(me * own, 128), own)
        load_g = pltpu.make_async_copy(out_grad.at[:, own_columns], g_buf.at[me], load_sem.at[0])
        load_a = pltpu.make_async_copy(act, a_buf.at[me], load_sem.at[1])

        def load_w(k):
            return pltpu.make_async_copy(weight.at[0, pl.ds(k * block, block)], w_buf.at[k % 2], w_sem.at[k % 2])

        load_w(0).start()
        load_w(1).start()
        load_g.start()
        load_a.start()
        pl.semaphore_wait(barrier, n_dp - 1 + 1 + n_col - 1)

        def g_span(which, h):
            return pl.ds(pl.multiple_of(which * quarter + h * g_rows, g_rows), g_rows)

        def send_g(target, h):
            columns = pl.ds(pl.multiple_of(target * own, 128), own)
            return remote(
                out_grad.at[g_span(col, h), columns], g_buf.at[me, g_span(col, h)],
                gz_send.at[target, h], g_recv.at[me, col, h], {"dp": target},
            )

        upper = me // (n_dp // 2)

        def at(position):
            return position + upper * (n_dp - 1 - 2 * position)

        toward = 1 - 2 * upper
        place = at(me)
        spot = [at(position) for position in range(n_dp)]
        started = ([], [])

        def go(role, make):
            make().start()
            started[role].append(make)

        def give_g(role, target):
            for h in range(halves):
                go(role, lambda h=h: send_g(target, h))

        @pl.when(place == 0)
        def _():
            give_g(0, spot[1])

        @pl.when(place == 1)
        def _():
            give_g(1, spot[2])
            give_g(1, spot[0])

        def a_span(which, h):
            return pl.ds(pl.multiple_of(which * half + h * a_rows, a_rows), a_rows)

        def send_a(source, inward, h, which, slot, own=False):
            span = a_span(which, h)
            return remote(
                act.at[span] if own else a_buf.at[source, span], a_buf.at[source, span],
                az_send.at[slot, inward, h], a_recv.at[source, which, h], {"dp": me + (2 * inward - 1) * toward},
            )

        def swap_a(source, h):
            span = a_span(row, h)
            return remote(
                a_buf.at[source, span], a_buf.at[source, span], ay_send.at[source, h], a_recv.at[source, row, h],
                {"row": partner},
            )

        def arrived_a(source, which, h):
            span = a_span(which, h)
            remote(
                a_buf.at[source, span], a_buf.at[source, span], ay_send.at[source, h], a_recv.at[source, which, h],
                {"row": partner},
            ).wait_recv()

        def give_a(role, inward):
            for h in range(halves):
                go(role, lambda h=h: send_a(me, inward, h, row, me, own=True))

        for k in range(own // 128):
            values = steps[0:1, pl.ds(pl.multiple_of(me * own + k * 128, 128), 128)]
            s_buf[pl.ds(k * 128, 128), :] = jnp.transpose(jnp.broadcast_to(values, (128, 128)))

        n_block = own // block

        for k in range(n_block):
            load_w(k).wait()
            s = jnp.concatenate([s_buf[pl.ds(k * block, block), :]] * (width // 128), axis=1)
            ratio = w_buf[k % 2] / s
            clipped = jnp.clip(ratio, -8.0, 7.0)
            levels = jnp.floor(clipped + 0.5)
            q_buf[pl.ds(k * block, block), :] = (levels * s).astype(jnp.bfloat16)
            f_buf[pl.ds(k * block, block), :] = jnp.where(clipped == ratio, levels - ratio, clipped).astype(jnp.bfloat16)
            if k + 2 < n_block:
                load_w(k + 2).start()
        load_g.wait()

        def dx_tile(d, start, size):
            return jnp.dot(
                g_buf[d, pl.ds(pl.multiple_of(start, size), size), :], q_buf[...], preferred_element_type=jnp.float32
            )

        def partial(d, i):
            part = pl.ds(pl.multiple_of(i * piece, piece), piece)
            return remote(p_send.at[d, part], p_recv.at[d, part], p_ssem.at[d, i], p_rsem.at[d, i], {"row": partner})

        def send_partials(d):
            def body(i, carry):
                p_send[d, pl.ds(pl.multiple_of(i * piece, piece), piece), :] = dx_tile(
                    d, partner * half + i * piece, piece
                ).astype(jnp.bfloat16)
                partial(d, i).start()
                return carry

            lax.fori_loop(0, pieces, body, 0)

        def add_products(d, first=False, last=False):
            def body(k, carry):
                rows = pl.ds(pl.multiple_of(k * block, block), block)
                new = lax.dot_general(
                    g_buf[d, :, rows], a_buf[d], (((0,), (0,)), ((), ())), preferred_element_type=jnp.float32
                )
                if not first:
                    new = new + prod[rows, :]
                if last:
                    factor = f_buf[rows, :].astype(jnp.float32)
                    prod[rows, :] = jnp.where(jnp.abs(factor) < 1.0, new, 0.0)
                    share = new * factor
                    lanes = share[:, 0:128]
                    for j in range(1, width // 128):
                        lanes = lanes + share[:, j * 128:(j + 1) * 128]
                    sg_buf[:, rows] = jnp.sum(jnp.transpose(lanes), axis=0, keepdims=True) * factor_scale
                else:
                    prod[rows, :] = new
                return carry

            lax.fori_loop(0, n_block, body, 0)

        send_partials(me)
        load_a.wait()
        add_products(me, first=True)

        def forward_g(d, differs, bit, slot, h):
            span = g_span(columns_by[differs], h)
            return remote(
                g_buf.at[d, span], g_buf.at[d, span], gx_send.at[d, slot, h], g_recv.at[d, columns_by[differs], h],
                {"col": columns_by[bit]},
            )

        def arrived_g(d, differs, h):
            forward_g(d, differs, bits[0], 0, h).wait_recv()

        def first_g(role, d, then=None):
            for h in range(halves):
                arrived_g(d, 0, h)
                for slot, bit in enumerate(bits):
                    go(role, lambda bit=bit, slot=slot, h=h: forward_g(d, 0, bit, slot, h))
                if h == 0 and then is not None:
                    then()

        def rest_g(role, d):
            slot, held = len(bits), [0]
            for b, bit in enumerate(bits):
                come = [differs ^ bit for differs in held]
                for differs in come:
                    later = bits[b + 1:]
                    for h in range(halves):
                        arrived_g(d, differs, h)
                        for j, over in enumerate(later):
                            go(role, lambda differs=differs, over=over, slot=slot + j, h=h: forward_g(d, differs, over, slot, h))
                    slot += len(later)
                held += come
            send_partials(d)

        def chain(d, slot, i, step):
            part = pl.ds(pl.multiple_of(i * piece, piece), piece)
            return remote(c_send.at[d, part], c_recv.at[slot, part], c_ssem.at[d, i], c_rsem.at[slot, i], {"dp": me + step})

        def own_sum(d, i):
            part = pl.ds(pl.multiple_of(i * piece, piece), piece)
            partial(d, i).wait_recv()
            acc[...] = dx_tile(d, row * half + i * piece, piece) + p_recv[d, part, :].astype(jnp.float32)

        def add_incoming(slot, i):
            part = pl.ds(pl.multiple_of(i * piece, piece), piece)
            remote(
                c_recv.at[slot, part], c_recv.at[slot, part], c_ssem.at[0, i], c_rsem.at[slot, i], {"row": partner}
            ).wait_recv()
            acc[...] = acc[...] + c_recv[slot, part, :].astype(jnp.float32)

        def pass_step(i, d, inward, first=False, last=False):
            step = toward * (2 * inward - 1)
            slot = d + (1 - step) // 2 * (n_dp - d) if last else d
            part = pl.ds(pl.multiple_of(i * piece, piece), piece)
            own_sum(d, i)
            if not first:
                add_incoming(d, i)
            c_send[d, part, :] = acc[...].astype(jnp.bfloat16)
            chain(d, slot, i, step).start()

        def pass_on(low, high, *jobs):
            def body(i, carry):
                for d, inward, lag, kind in jobs:
                    pass_step(i - lag, d, inward, **kind)
                return carry

            lax.fori_loop(low, high, body, 0)

        def take_a(role, d, onward=(), swaps=tuple(range(halves)), parts=tuple(range(halves))):
            for h in parts:
                arrived_a(d, row, h)
                for inward in onward:
                    go(role, lambda inward=inward, h=h: send_a(d, inward, h, row, d))
                if h in swaps:
                    go(role, lambda h=h: swap_a(d, h))

        def products_of(d, last=False, skip=()):
            for h in range(halves):
                if h not in skip:
                    arrived_a(d, partner, h)
            add_products(d, last=last)

        def finish():
            def body(i, carry):
                part = pl.ds(pl.multiple_of(i * piece, piece), piece)
                own_sum(me, i)

                @pl.when(me > 0)
                def _():
                    add_incoming(me, i)

                @pl.when(me < n_dp - 1)
                def _():
                    add_incoming(n_dp, i)

                input_grad[part, :] = acc[...].astype(jnp.bfloat16)
                return carry

            lax.fori_loop(0, pieces, body, 0)

        def swap_steps(differs):
            return remote(
                sg_buf, sg_in.at[differs - 1], sg_ssem.at[differs - 1], sg_rsem.at[differs - 1],
                {"col": columns_by[differs]},
            )

        def give_steps(role):
            for differs in range(1, n_col):
                go(role, lambda differs=differs: swap_steps(differs))

        start, end, split = dict(first=True), dict(last=True), pieces // 2

        @pl.when(place == 0)
        def _():
            r = 0
            first_g(r, spot[1], lambda: give_g(r, spot[2]))
            rest_g(r, spot[1])
            give_a(r, 1)
            first_g(r, spot[2], lambda: give_g(r, spot[3]))
            take_a(r, spot[1], swaps=(0,))
            go(r, lambda: send_a(me, 1, 0, partner, n_dp, own=True))
            rest_g(r, spot[2])
            first_g(r, spot[3])
            rest_g(r, spot[3])
            pass_on(0, split, (spot[2], 1, 0, start))
            pass_on(0, pieces - 1, (spot[3], 1, 0, start))
            take_a(r, spot[2], swaps=(1,))
            pass_on(pieces - 1, pieces, (spot[3], 1, 0, start))
            pass_on(split, pieces, (spot[2], 1, 0, start))
            pass_on(0, pieces, (spot[1], 1, 0, dict(first=True, last=True)))
            products_of(spot[1])
            take_a(r, spot[3])
            products_of(spot[2])
            products_of(spot[3], last=True)
            give_steps(r)
            finish()

        @pl.when(place == 1)
        def _():
            r = 1
            first_g(r, spot[0], lambda: give_a(r, 0))
            first_g(r, spot[2])
            give_g(r, spot[3])
            rest_g(r, spot[0])
            first_g(r, spot[3])
            rest_g(r, spot[2])
            give_a(r, 1)
            rest_g(r, spot[3])
            go(r, lambda: send_a(me, 0, 1, partner, n_dp, own=True))
            take_a(r, spot[0], (1,), swaps=(1,))
            take_a(r, spot[2], (0,))
            take_a(r, spot[3], (0,), parts=(0,))
            pass_on(0, split, (spot[2], 1, 0, end))
            products_of(spot[0])
            take_a(r, spot[3], (0,), parts=(1,))
            pass_on(0, 1, (spot[3], 1, 0, {}))
            arrived_a(spot[2], partner, 0)
            go(r, lambda: send_a(spot[2], 0, 0, partner, n_dp))
            pass_on(1, split, (spot[3], 1, 0, {}))
            products_of(spot[2], skip=(0,))
            pass_on(split, pieces, (spot[3], 1, 0, {}), (spot[0], 0, split, end))
            pass_on(split, pieces - 1, (spot[0], 0, 0, end))
            pass_on(split, pieces, (spot[2], 1, 0, end))
            pass_on(pieces - 1, pieces, (spot[0], 0, 0, end))
            products_of(spot[3], last=True)
            give_steps(r)
            finish()

        for differs in range(1, n_col):
            swap_steps(differs).wait_recv()
        total = sg_buf[...]
        for differs in range(1, n_col):
            total = total + sg_in[differs - 1]
        step_grad[...] = total

        for role in range(2):
            @pl.when(place == role)
            def _():
                for make in started[role]:
                    make().wait_send()

        def drain(d, carry):
            def each(i, inner):
                partial(d, i).wait_send()

                @pl.when(me != d)
                def _():
                    part = pl.ds(pl.multiple_of(i * piece, piece), piece)
                    remote(
                        c_send.at[d, part], c_send.at[d, part], c_ssem.at[d, i], c_rsem.at[d, i], {"row": partner}
                    ).wait_send()

                return inner

            return lax.fori_loop(0, pieces, each, carry)

        lax.fori_loop(0, n_dp, drain, 0)
    scratch = [
        pltpu.VMEM((n_dp, tokens, own), jnp.bfloat16),
        pltpu.VMEM((n_dp, tokens, width), jnp.bfloat16),
        pltpu.VMEM((own, width), jnp.bfloat16),
        pltpu.VMEM((own, width), jnp.bfloat16),
        pltpu.VMEM((n_dp, half, width), jnp.bfloat16),
        pltpu.VMEM((n_dp, half, width), jnp.bfloat16),
        pltpu.VMEM((n_dp, half, width), jnp.bfloat16),
        pltpu.VMEM((n_dp + 1, half, width), jnp.bfloat16),
        pltpu.VMEM((2, block, width), jnp.float32),
        pltpu.VMEM((own, 128), jnp.float32),
        pltpu.VMEM((piece, width), jnp.float32),
        pltpu.VMEM((1, own), jnp.float32),
        pltpu.VMEM((n_col - 1, 1, own), jnp.float32),
        pltpu.SemaphoreType.DMA((2,)),
        pltpu.SemaphoreType.DMA((2,)),
        pltpu.SemaphoreType.DMA((n_dp, halves)),
        pltpu.SemaphoreType.DMA((n_dp, n_col, halves)),
        pltpu.SemaphoreType.DMA((n_dp, n_col - 1, halves)),
        pltpu.SemaphoreType.DMA((n_dp + 1, 2, halves)),
        pltpu.SemaphoreType.DMA((n_dp, halves)),
        pltpu.SemaphoreType.DMA((n_dp, n_row, halves)),
        pltpu.SemaphoreType.DMA((n_dp, pieces)),
        pltpu.SemaphoreType.DMA((n_dp, pieces)),
        pltpu.SemaphoreType.DMA((n_dp, pieces)),
        pltpu.SemaphoreType.DMA((n_dp + 1, pieces)),
        pltpu.SemaphoreType.DMA((n_col - 1,)),
        pltpu.SemaphoreType.DMA((n_col - 1,)),
    ]
    anywhere = pl.BlockSpec(memory_space=pl.ANY)
    inside = pl.BlockSpec(memory_space=pltpu.VMEM)
    return pl.pallas_call(
        kernel,
        out_shape=(
            pltpu.VMEM((half, width), jnp.bfloat16),
            pltpu.VMEM((1, own, width), jnp.float32),
            pltpu.VMEM((1, own), jnp.float32),
        ),
        in_specs=[anywhere, anywhere, anywhere, inside],
        out_specs=(inside, inside, inside),
        scratch_shapes=scratch,
        compiler_params=pltpu.CompilerParams(collective_id=0, has_side_effects=True, vmem_limit_bytes=55 * 2**20),
        name="backward",
    )


def fits(n_dp, n_row, n_col, activations, weight):
    tokens, width = activations.shape
    own = weight.shape[1]
    return (
        n_dp == 4 and n_row == 2 and n_col > 1 and n_col & (n_col - 1) == 0
        and own % 256 == 0 and width % 128 == 0 and tokens % (128 * n_row) == 0 and tokens % (32 * n_col) == 0
        and n_dp * tokens * (own + width) <= 12 * 2**20
    )


def solution(mesh):
    n_dp, n_row, n_col = mesh.shape["dp"], mesh.shape["row"], mesh.shape["col"]
    in_specs = (P("dp", "col"), P("dp", "row"), P("row", "dp", "col"), P("row", None))
    out_specs = (P(("dp", "row"), "col"), P("row", "dp", "col"), P("row", "dp"))
    general = make_shards(n_dp, n_row, n_col)

    def shards(activations, out_grad, weight, step_size):
        if not fits(n_dp, n_row, n_col, activations, weight):
            return general(activations, out_grad, weight, step_size)
        tokens, width = activations.shape
        call = make_kernel(n_dp, n_row, n_col, tokens, weight.shape[1], width)
        return call(activations, out_grad, weight, step_size)

    return jax.shard_map(shards, mesh=mesh, in_specs=in_specs, out_specs=out_specs, check_vma=False)
```

```python
import jax
import jax.numpy as jnp
from jax import lax
from jax.experimental.layout import Layout, with_layout_constraint
from jax.experimental import pallas as pl
from jax.experimental.pallas import tpu as pltpu
from jax.sharding import PartitionSpec as P

D = 4096


def quantize(latent, scales):
    ratio = latent / scales[:, None]
    clipped = jnp.clip(ratio, -8.0, 7.0)
    levels = jnp.floor(clipped + 0.5)
    inside = jnp.where((ratio >= -8.0) & (ratio <= 7.0), 1.0, 0.0).astype(jnp.float32)
    factor = jnp.where(inside > 0.5, levels - ratio, clipped)
    quantized = (levels * scales[:, None]).astype(jnp.bfloat16)
    return (quantized, inside, factor)


def shift(block, axis, count, by):
    return lax.ppermute(block, axis, [(i, (i + by) % count) for i in range(count)])


def swap(block, axis, count, bit):
    return lax.ppermute(block, axis, [(i, i ^ bit) for i in range(count)])


def gather_rows(block, axis, count):
    position = lax.axis_index(axis)
    bit = 1
    bits = []
    while bit < count:
        bits.append(bit)
        bit *= 2
    pieces = {0: block}
    for bit in reversed(bits):
        held = dict(pieces)
        for key in held:
            pieces[key ^ bit] = swap(held[key], axis, count, bit)
    parts = [pieces[key] for key in range(count)]
    for bit in bits:
        flag = (position & bit) != 0
        parts = [
            jnp.where(flag, parts[key ^ bit], parts[key]) for key in range(count)
        ]
    return jnp.concatenate(parts, axis=0)


def make_shards(n_dp, n_row, n_col):
    def shards(activations, out_grad, weight, step_size):
        own_count = weight.shape[1]
        tokens = out_grad.shape[0]
        dp = lax.axis_index("dp")
        row = lax.axis_index("row")
        col = lax.axis_index("col")
        scales = step_size[0]
        own_scales = lax.dynamic_slice_in_dim(scales, dp * own_count, own_count, 0)
        grad_factor = 1.0 / (7.0 * D) ** 0.5

        share = tokens // n_col
        half = tokens // n_row
        mine = lax.dynamic_slice_in_dim(out_grad, col * share, share, 0)
        ring = lax.dynamic_slice_in_dim(activations, row * half, half, 0)
        grads, acts = [], []
        for k in range(1, n_dp):
            target = (dp + k) % n_dp
            chunk = lax.dynamic_slice_in_dim(mine, target * own_count, own_count, 1)
            grads.append(shift(chunk, "dp", n_dp, k))
            ring = shift(ring, "dp", n_dp, 1)
            acts.append(ring)

        quantized, _, _ = quantize(weight[0], own_scales)
        own_grad = lax.dynamic_slice_in_dim(out_grad, dp * own_count, own_count, 1)

        def reduced(grad):
            size = tokens
            bit = n_row // 2
            if bit == 0:
                return jnp.dot(grad, quantized, preferred_element_type=jnp.float32)
            size //= 2
            upper = ((row // bit) % 2).astype(jnp.int32)
            sent = lax.dynamic_slice_in_dim(grad, (1 - upper) * size, size, 0)
            kept = lax.dynamic_slice_in_dim(grad, upper * size, size, 0)
            out = jnp.dot(sent, quantized, preferred_element_type=jnp.float32).astype(jnp.bfloat16)
            came = swap(out, "row", n_row, bit)
            total = jnp.dot(kept, quantized, preferred_element_type=jnp.float32) + came.astype(jnp.float32)
            bit //= 2
            while bit:
                size //= 2
                upper = (row // bit) % 2 == 1
                low, high = total[:size], total[size:]
                came = swap(jnp.where(upper, low, high).astype(jnp.bfloat16), "row", n_row, bit)
                total = jnp.where(upper, high, low) + came.astype(jnp.float32)
                bit //= 2
            return total

        products = lax.dot_general(
            own_grad, activations, (((0,), (0,)), ((), ())), preferred_element_type=jnp.float32
        )
        own_total = reduced(own_grad)
        if grads:
            grads[0], quantized, products = lax.optimization_barrier((grads[0], quantized, products))
        running = None
        for k in range(1, n_dp):
            grad = gather_rows(grads[k - 1], "col", n_col)
            total = reduced(grad)
            if running is not None:
                total = total + running.astype(jnp.float32)
            leaving, grad = lax.optimization_barrier((total.astype(jnp.bfloat16), grad))
            running = shift(leaving, "dp", n_dp, 1)
            act = gather_rows(acts[k - 1], "row", n_row)
            products = products + lax.dot_general(
                grad, act, (((0,), (0,)), ((), ())), preferred_element_type=jnp.float32
            )
        if running is not None:
            own_total = own_total + running.astype(jnp.float32)
        products, latent = lax.optimization_barrier((products, weight[0]))
        products = with_layout_constraint(products, Layout((0, 1)))
        _, inside, factor = quantize(latent, own_scales)
        input_grad = own_total.astype(jnp.bfloat16)
        step_rows = lax.psum(jnp.sum(products * factor, axis=1) * grad_factor, "col")
        weight_grad = (products * inside)[None]
        return (input_grad, weight_grad, step_rows[None])

    return shards


MESH = pl.DeviceIdType.MESH


def flipped(position, bit):
    return position + bit * (1 - 2 * lax.rem(position // bit, 2))


def make_kernel(n_dp, n_row, n_col, tokens, own, width):
    quarter = tokens // n_col
    half = tokens // n_row
    piece = 128
    pieces = half // piece
    block = 256
    halves = 2
    g_rows = quarter // halves
    parts = 4
    a_rows = half // parts
    block_pieces = quarter // piece
    factor_scale = 1.0 / (7.0 * width * n_col) ** 0.5
    bits = []
    bit = n_col // 2
    while bit:
        bits.append(bit)
        bit //= 2

    def kernel(act, out_grad, weight, steps, input_grad, weight_grad, step_grad,
               g_buf, a_buf, q_buf, f_buf, p_send, p_recv, c_send, c_recv, w_buf, s_buf, acc, sg_buf, sg_in,
               load_sem, w_sem, gz_send, g_recv, gx_send, az_send, ay_send, a_recv,
               p_ssem, p_rsem, c_ssem, c_rsem, sg_ssem, sg_rsem):
        prod = weight_grad.at[0]
        me = lax.axis_index("dp")
        row = lax.axis_index("row")
        col = lax.axis_index("col")
        partner = 1 - row

        def remote(src, dst, send, recv, where):
            return pltpu.make_async_remote_copy(
                src_ref=src, dst_ref=dst, send_sem=send, recv_sem=recv, device_id=where, device_id_type=MESH
            )

        def rows_of(index, size):
            return pl.ds(pl.multiple_of(index * size, size), size)

        barrier = pltpu.get_barrier_semaphore()
        for k in range(1, n_dp):
            pl.semaphore_signal(barrier, inc=1, device_id={"dp": lax.rem(me + k, n_dp)}, device_id_type=MESH)
        pl.semaphore_signal(barrier, inc=1, device_id={"row": partner}, device_id_type=MESH)
        columns_by = [col]
        for bit in reversed(bits):
            columns_by += [flipped(which, bit) for which in columns_by]
        for which in columns_by[1:]:
            pl.semaphore_signal(barrier, inc=1, device_id={"col": which}, device_id_type=MESH)

        own_columns = pl.ds(pl.multiple_of(me * own, 128), own)
        load_g = pltpu.make_async_copy(out_grad.at[:, own_columns], g_buf.at[me], load_sem.at[0])
        load_a = pltpu.make_async_copy(act, a_buf.at[me], load_sem.at[1])

        def load_w(k):
            return pltpu.make_async_copy(weight.at[0, pl.ds(k * block, block)], w_buf.at[k % 2], w_sem.at[k % 2])

        load_w(0).start()
        load_w(1).start()
        load_g.start()
        load_a.start()
        pl.semaphore_wait(barrier, n_dp - 1 + 1 + n_col - 1)

        def g_span(which, h):
            dealt = lax.rem(which, 2) * (n_col // 2) + which // 2
            return pl.ds(pl.multiple_of(dealt * quarter + h * g_rows, g_rows), g_rows)

        def nth(i):
            return lax.rem(i + col // 2 * block_pieces, pieces)

        def send_g(target, h):
            columns = pl.ds(pl.multiple_of(target * own, 128), own)
            return remote(
                out_grad.at[g_span(col, h), columns], g_buf.at[me, g_span(col, h)],
                gz_send.at[target, h], g_recv.at[me, col, h], {"dp": target},
            )

        upper = me // (n_dp // 2)

        def at(position):
            return position + upper * (n_dp - 1 - 2 * position)

        toward = 1 - 2 * upper
        place = at(me)
        spot = [at(position) for position in range(n_dp)]
        started = ([], [])

        def go(role, make):
            make().start()
            started[role].append(make)

        def give_g(role, target):
            for h in range(halves):
                go(role, lambda h=h: send_g(target, h))

        @pl.when(place == 0)
        def _():
            give_g(0, spot[1])

        @pl.when(place == 1)
        def _():
            give_g(1, spot[2])
            give_g(1, spot[0])

        def a_span(which, h):
            return pl.ds(pl.multiple_of(which * half + h * a_rows, a_rows), a_rows)

        def send_a(source, inward, h, which, slot, own=False):
            span = a_span(which, h)
            return remote(
                act.at[span] if own else a_buf.at[source, span], a_buf.at[source, span],
                az_send.at[slot, inward, h], a_recv.at[source, which, h], {"dp": me + (2 * inward - 1) * toward},
            )

        def swap_a(source, h):
            span = a_span(row, h)
            return remote(
                a_buf.at[source, span], a_buf.at[source, span], ay_send.at[source, h], a_recv.at[source, row, h],
                {"row": partner},
            )

        def arrived_a(source, which, h):
            span = a_span(which, h)
            remote(
                a_buf.at[source, span], a_buf.at[source, span], ay_send.at[source, h], a_recv.at[source, which, h],
                {"row": partner},
            ).wait_recv()

        def give_a(role, inward):
            for h in range(parts):
                go(role, lambda h=h: send_a(me, inward, h, row, me, own=True))

        for k in range(own // 128):
            values = steps[0:1, pl.ds(pl.multiple_of(me * own + k * 128, 128), 128)]
            s_buf[pl.ds(k * 128, 128), :] = jnp.transpose(jnp.broadcast_to(values, (128, 128)))

        n_block = own // block

        for k in range(n_block):
            load_w(k).wait()
            s = jnp.concatenate([s_buf[pl.ds(k * block, block), :]] * (width // 128), axis=1)
            ratio = w_buf[k % 2] / s
            clipped = jnp.clip(ratio, -8.0, 7.0)
            levels = jnp.floor(clipped + 0.5)
            q_buf[pl.ds(k * block, block), :] = (levels * s).astype(jnp.bfloat16)
            f_buf[pl.ds(k * block, block), :] = jnp.where(clipped == ratio, levels - ratio, clipped).astype(jnp.bfloat16)
            if k + 2 < n_block:
                load_w(k + 2).start()
        load_g.wait()

        def dx_tile(d, start, size):
            return jnp.dot(
                g_buf[d, pl.ds(pl.multiple_of(start, size), size), :], q_buf[...], preferred_element_type=jnp.float32
            )

        def partial(d, i):
            part = pl.ds(pl.multiple_of(i * piece, piece), piece)
            return remote(p_send.at[d, part], p_recv.at[d, part], p_ssem.at[d, i], p_rsem.at[d, i], {"row": partner})

        def send_partials(d, low=0, high=pieces):
            def body(k, carry):
                i = nth(k)
                p_send[d, pl.ds(pl.multiple_of(i * piece, piece), piece), :] = dx_tile(
                    d, partner * half + i * piece, piece
                ).astype(jnp.bfloat16)
                partial(d, i).start()
                return carry

            lax.fori_loop(low, high, body, 0)

        def add_products(d, first=False, last=False):
            def body(k, carry):
                rows = pl.ds(pl.multiple_of(k * block, block), block)
                new = lax.dot_general(
                    g_buf[d, :, rows], a_buf[d], (((0,), (0,)), ((), ())), preferred_element_type=jnp.float32
                )
                if not first:
                    new = new + prod[rows, :]
                if last:
                    factor = f_buf[rows, :].astype(jnp.float32)
                    prod[rows, :] = jnp.where(jnp.abs(factor) < 1.0, new, 0.0)
                    share = new * factor
                    lanes = share[:, 0:128]
                    for j in range(1, width // 128):
                        lanes = lanes + share[:, j * 128:(j + 1) * 128]
                    sg_buf[:, rows] = jnp.sum(jnp.transpose(lanes), axis=0, keepdims=True) * factor_scale
                else:
                    prod[rows, :] = new
                return carry

            lax.fori_loop(0, n_block, body, 0)

        send_partials(me)
        load_a.wait()
        add_products(me, first=True)

        def forward_g(d, differs, bit, slot, h):
            span = g_span(columns_by[differs], h)
            return remote(
                g_buf.at[d, span], g_buf.at[d, span], gx_send.at[d, slot, h], g_recv.at[d, columns_by[differs], h],
                {"col": columns_by[bit]},
            )

        def arrived_g(d, differs, h):
            forward_g(d, differs, bits[0], 0, h).wait_recv()

        def first_g(role, d, then=None):
            for h in range(halves):
                arrived_g(d, 0, h)
                for slot, bit in enumerate(bits):
                    go(role, lambda bit=bit, slot=slot, h=h: forward_g(d, 0, bit, slot, h))
                if h == 0 and then is not None:
                    then()

        def early_g(d):
            for h in range(halves):
                arrived_g(d, 1, h)
            send_partials(d, 0, block_pieces)

        def rest_g(role, d):
            slot, held = len(bits), [0]
            for b, bit in enumerate(bits):
                come = [differs ^ bit for differs in held]
                for differs in come:
                    later = bits[b + 1:]
                    for h in range(halves):
                        if differs != 1:
                            arrived_g(d, differs, h)
                        for j, over in enumerate(later):
                            go(role, lambda differs=differs, over=over, slot=slot + j, h=h: forward_g(d, differs, over, slot, h))
                    slot += len(later)
                held += come
            send_partials(d, block_pieces)

        def chain(d, slot, i, step):
            part = pl.ds(pl.multiple_of(i * piece, piece), piece)
            return remote(c_send.at[d, part], c_recv.at[slot, part], c_ssem.at[d, i], c_rsem.at[slot, i], {"dp": me + step})

        def own_sum(d, i):
            part = pl.ds(pl.multiple_of(i * piece, piece), piece)
            partial(d, i).wait_recv()
            acc[...] = dx_tile(d, row * half + i * piece, piece) + p_recv[d, part, :].astype(jnp.float32)

        def add_incoming(slot, i):
            part = pl.ds(pl.multiple_of(i * piece, piece), piece)
            remote(
                c_recv.at[slot, part], c_recv.at[slot, part], c_ssem.at[0, i], c_rsem.at[slot, i], {"row": partner}
            ).wait_recv()
            acc[...] = acc[...] + c_recv[slot, part, :].astype(jnp.float32)

        def pass_step(i, d, inward, first=False, last=False):
            step = toward * (2 * inward - 1)
            slot = d + (1 - step) // 2 * (n_dp - d) if last else d
            part = pl.ds(pl.multiple_of(i * piece, piece), piece)
            own_sum(d, i)
            if not first:
                add_incoming(d, i)
            c_send[d, part, :] = acc[...].astype(jnp.bfloat16)
            chain(d, slot, i, step).start()

        def pass_on(low, high, *jobs):
            def body(i, carry):
                for d, inward, lag, kind in jobs:
                    pass_step(nth(i - lag), d, inward, **kind)
                return carry

            lax.fori_loop(low, high, body, 0)

        def take_a(role, d, onward=(), swaps=tuple(range(parts)), which=tuple(range(parts))):
            for h in which:
                arrived_a(d, row, h)
                for inward in onward:
                    go(role, lambda inward=inward, h=h: send_a(d, inward, h, row, d))
                if h in swaps:
                    go(role, lambda h=h: swap_a(d, h))

        def products_of(d, last=False, skip=()):
            for h in range(parts):
                if h not in skip:
                    arrived_a(d, partner, h)
            add_products(d, last=last)

        def finish():
            def body(k, carry):
                i = nth(k)
                part = pl.ds(pl.multiple_of(i * piece, piece), piece)
                own_sum(me, i)

                @pl.when(me > 0)
                def _():
                    add_incoming(me, i)

                @pl.when(me < n_dp - 1)
                def _():
                    add_incoming(n_dp, i)

                input_grad[part, :] = acc[...].astype(jnp.bfloat16)
                return carry

            lax.fori_loop(0, pieces, body, 0)

        def swap_steps(differs):
            return remote(
                sg_buf, sg_in.at[differs - 1], sg_ssem.at[differs - 1], sg_rsem.at[differs - 1],
                {"col": columns_by[differs]},
            )

        def give_steps(role):
            for differs in range(1, n_col):
                go(role, lambda differs=differs: swap_steps(differs))

        start, end, split = dict(first=True), dict(last=True), pieces // 2
        low, high = tuple(range(parts // 2)), tuple(range(parts // 2, parts))

        @pl.when(place == 0)
        def _():
            r = 0
            first_g(r, spot[1], lambda: give_g(r, spot[2]))
            early_g(spot[1])
            rest_g(r, spot[1])
            give_a(r, 1)

            def meanwhile():
                give_g(r, spot[3])
                take_a(r, spot[1], which=low)

            first_g(r, spot[2], meanwhile)
            early_g(spot[2])
            for h in low:
                go(r, lambda h=h: send_a(me, 1, h, partner, n_dp, own=True))
            rest_g(r, spot[2])
            first_g(r, spot[3])
            early_g(spot[3])
            rest_g(r, spot[3])
            pass_on(0, split, (spot[2], 1, 0, start))
            pass_on(0, pieces - 1, (spot[3], 1, 0, start))
            take_a(r, spot[2], swaps=tuple(range(1, parts)))
            pass_on(pieces - 1, pieces, (spot[3], 1, 0, start))
            pass_on(split, pieces, (spot[2], 1, 0, start))
            pass_on(0, pieces, (spot[1], 1, 0, dict(first=True, last=True)))
            take_a(r, spot[3], which=low)
            take_a(r, spot[1], swaps=(), which=high)
            products_of(spot[1])
            take_a(r, spot[3], which=high)
            products_of(spot[2])
            products_of(spot[3], last=True)
            give_steps(r)
            finish()

        @pl.when(place == 1)
        def _():
            r = 1
            first_g(r, spot[0], lambda: give_a(r, 0))
            first_g(r, spot[2])
            give_g(r, spot[3])
            early_g(spot[0])
            early_g(spot[2])
            rest_g(r, spot[0])
            first_g(r, spot[3])
            early_g(spot[3])
            rest_g(r, spot[2])
            give_a(r, 1)
            rest_g(r, spot[3])
            for h in high:
                go(r, lambda h=h: send_a(me, 0, h, partner, n_dp, own=True))
            take_a(r, spot[0], (1,), swaps=high)
            take_a(r, spot[2], (0,))
            take_a(r, spot[3], (0,), which=low)
            pass_on(0, split, (spot[2], 1, 0, end))
            products_of(spot[0])
            take_a(r, spot[3], (0,), which=high)
            pass_on(0, 1, (spot[3], 1, 0, {}))
            arrived_a(spot[2], partner, 0)
            go(r, lambda: send_a(spot[2], 0, 0, partner, n_dp))
            pass_on(1, split, (spot[3], 1, 0, {}))
            products_of(spot[2], skip=(0,))
            pass_on(split, pieces, (spot[3], 1, 0, {}), (spot[0], 0, split, end))
            pass_on(split, pieces - 1, (spot[0], 0, 0, end))
            pass_on(split, pieces, (spot[2], 1, 0, end))
            pass_on(pieces - 1, pieces, (spot[0], 0, 0, end))
            products_of(spot[3], last=True)
            give_steps(r)
            finish()

        for differs in range(1, n_col):
            swap_steps(differs).wait_recv()
        total = sg_buf[...]
        for differs in range(1, n_col):
            total = total + sg_in[differs - 1]
        step_grad[...] = total

        for role in range(2):
            @pl.when(place == role)
            def _():
                for make in started[role]:
                    make().wait_send()

        def drain(d, carry):
            def each(i, inner):
                partial(d, i).wait_send()

                @pl.when(me != d)
                def _():
                    part = pl.ds(pl.multiple_of(i * piece, piece), piece)
                    remote(
                        c_send.at[d, part], c_send.at[d, part], c_ssem.at[d, i], c_rsem.at[d, i], {"row": partner}
                    ).wait_send()

                return inner

            return lax.fori_loop(0, pieces, each, carry)

        lax.fori_loop(0, n_dp, drain, 0)
    scratch = [
        pltpu.VMEM((n_dp, tokens, own), jnp.bfloat16),
        pltpu.VMEM((n_dp, tokens, width), jnp.bfloat16),
        pltpu.VMEM((own, width), jnp.bfloat16),
        pltpu.VMEM((own, width), jnp.bfloat16),
        pltpu.VMEM((n_dp, half, width), jnp.bfloat16),
        pltpu.VMEM((n_dp, half, width), jnp.bfloat16),
        pltpu.VMEM((n_dp, half, width), jnp.bfloat16),
        pltpu.VMEM((n_dp + 1, half, width), jnp.bfloat16),
        pltpu.VMEM((2, block, width), jnp.float32),
        pltpu.VMEM((own, 128), jnp.float32),
        pltpu.VMEM((piece, width), jnp.float32),
        pltpu.VMEM((1, own), jnp.float32),
        pltpu.VMEM((n_col - 1, 1, own), jnp.float32),
        pltpu.SemaphoreType.DMA((2,)),
        pltpu.SemaphoreType.DMA((2,)),
        pltpu.SemaphoreType.DMA((n_dp, halves)),
        pltpu.SemaphoreType.DMA((n_dp, n_col, halves)),
        pltpu.SemaphoreType.DMA((n_dp, n_col - 1, halves)),
        pltpu.SemaphoreType.DMA((n_dp + 1, 2, parts)),
        pltpu.SemaphoreType.DMA((n_dp, parts)),
        pltpu.SemaphoreType.DMA((n_dp, n_row, parts)),
        pltpu.SemaphoreType.DMA((n_dp, pieces)),
        pltpu.SemaphoreType.DMA((n_dp, pieces)),
        pltpu.SemaphoreType.DMA((n_dp, pieces)),
        pltpu.SemaphoreType.DMA((n_dp + 1, pieces)),
        pltpu.SemaphoreType.DMA((n_col - 1,)),
        pltpu.SemaphoreType.DMA((n_col - 1,)),
    ]
    anywhere = pl.BlockSpec(memory_space=pl.ANY)
    inside = pl.BlockSpec(memory_space=pltpu.VMEM)
    return pl.pallas_call(
        kernel,
        out_shape=(
            pltpu.VMEM((half, width), jnp.bfloat16),
            pltpu.VMEM((1, own, width), jnp.float32),
            pltpu.VMEM((1, own), jnp.float32),
        ),
        in_specs=[anywhere, anywhere, anywhere, inside],
        out_specs=(inside, inside, inside),
        scratch_shapes=scratch,
        compiler_params=pltpu.CompilerParams(collective_id=0, has_side_effects=True, vmem_limit_bytes=55 * 2**20),
        name="backward",
    )


def leave(input_grad, weight_grad, step_grad):
    held = (input_grad, weight_grad, step_grad)
    cuts = 8
    rows = weight_grad.shape[1] // cuts

    def kernel(a, b, c, a_out, b_out, c_out, sems):
        copies = [pltpu.make_async_copy(a, a_out, sems.at[cuts]), pltpu.make_async_copy(c, c_out, sems.at[cuts + 1])]
        for k in range(cuts):
            span = pl.ds(k * rows, rows)
            copies.append(pltpu.make_async_copy(b.at[:, span], b_out.at[:, span], sems.at[k]))
        for copy in copies:
            copy.start()
        for copy in copies:
            copy.wait()

    return pl.pallas_call(
        kernel,
        out_shape=tuple(jax.ShapeDtypeStruct(x.shape, x.dtype) for x in held),
        in_specs=[pl.BlockSpec(memory_space=pltpu.VMEM)] * len(held),
        out_specs=tuple(pl.BlockSpec(memory_space=pl.ANY) for _ in held),
        scratch_shapes=[pltpu.SemaphoreType.DMA((cuts + 2,))],
        compiler_params=pltpu.CompilerParams(vmem_limit_bytes=2**20),
        name="leave",
    )(*(pltpu.with_memory_space_constraint(x, pltpu.VMEM) for x in held))


def fits(n_dp, n_row, n_col, activations, weight):
    tokens, width = activations.shape
    own = weight.shape[1]
    return (
        n_dp == 4 and n_row == 2 and n_col > 1 and n_col & (n_col - 1) == 0
        and own % 256 == 0 and width % 128 == 0 and tokens % (256 * n_row) == 0 and tokens % (128 * n_col) == 0
        and n_dp * tokens * (own + width) <= 12 * 2**20
    )


def solution(mesh):
    n_dp, n_row, n_col = mesh.shape["dp"], mesh.shape["row"], mesh.shape["col"]
    in_specs = (P("dp", "col"), P("dp", "row"), P("row", "dp", "col"), P("row", None))
    out_specs = (P(("dp", "row"), "col"), P("row", "dp", "col"), P("row", "dp"))
    general = make_shards(n_dp, n_row, n_col)

    def shards(activations, out_grad, weight, step_size):
        if not fits(n_dp, n_row, n_col, activations, weight):
            return general(activations, out_grad, weight, step_size)
        tokens, width = activations.shape
        call = make_kernel(n_dp, n_row, n_col, tokens, weight.shape[1], width)
        return leave(*call(activations, out_grad, weight, step_size))

    return jax.shard_map(shards, mesh=mesh, in_specs=in_specs, out_specs=out_specs, check_vma=False)
```

```python
import jax
import jax.numpy as jnp
from jax import lax
from jax.experimental.layout import Layout, with_layout_constraint
from jax.experimental import pallas as pl
from jax.experimental.pallas import tpu as pltpu
from jax.sharding import PartitionSpec as P

D = 4096


def quantize(latent, scales):
    ratio = latent / scales[:, None]
    clipped = jnp.clip(ratio, -8.0, 7.0)
    levels = jnp.floor(clipped + 0.5)
    inside = jnp.where((ratio >= -8.0) & (ratio <= 7.0), 1.0, 0.0).astype(jnp.float32)
    factor = jnp.where(inside > 0.5, levels - ratio, clipped)
    quantized = (levels * scales[:, None]).astype(jnp.bfloat16)
    return (quantized, inside, factor)


def shift(block, axis, count, by):
    return lax.ppermute(block, axis, [(i, (i + by) % count) for i in range(count)])


def swap(block, axis, count, bit):
    return lax.ppermute(block, axis, [(i, i ^ bit) for i in range(count)])


def gather_rows(block, axis, count):
    position = lax.axis_index(axis)
    bit = 1
    bits = []
    while bit < count:
        bits.append(bit)
        bit *= 2
    pieces = {0: block}
    for bit in reversed(bits):
        held = dict(pieces)
        for key in held:
            pieces[key ^ bit] = swap(held[key], axis, count, bit)
    parts = [pieces[key] for key in range(count)]
    for bit in bits:
        flag = (position & bit) != 0
        parts = [
            jnp.where(flag, parts[key ^ bit], parts[key]) for key in range(count)
        ]
    return jnp.concatenate(parts, axis=0)


def make_shards(n_dp, n_row, n_col):
    def shards(activations, out_grad, weight, step_size):
        own_count = weight.shape[1]
        tokens = out_grad.shape[0]
        dp = lax.axis_index("dp")
        row = lax.axis_index("row")
        col = lax.axis_index("col")
        scales = step_size[0]
        own_scales = lax.dynamic_slice_in_dim(scales, dp * own_count, own_count, 0)
        grad_factor = 1.0 / (7.0 * D) ** 0.5

        share = tokens // n_col
        half = tokens // n_row
        mine = lax.dynamic_slice_in_dim(out_grad, col * share, share, 0)
        ring = lax.dynamic_slice_in_dim(activations, row * half, half, 0)
        grads, acts = [], []
        for k in range(1, n_dp):
            target = (dp + k) % n_dp
            chunk = lax.dynamic_slice_in_dim(mine, target * own_count, own_count, 1)
            grads.append(shift(chunk, "dp", n_dp, k))
            ring = shift(ring, "dp", n_dp, 1)
            acts.append(ring)

        quantized, _, _ = quantize(weight[0], own_scales)
        own_grad = lax.dynamic_slice_in_dim(out_grad, dp * own_count, own_count, 1)

        def reduced(grad):
            size = tokens
            bit = n_row // 2
            if bit == 0:
                return jnp.dot(grad, quantized, preferred_element_type=jnp.float32)
            size //= 2
            upper = ((row // bit) % 2).astype(jnp.int32)
            sent = lax.dynamic_slice_in_dim(grad, (1 - upper) * size, size, 0)
            kept = lax.dynamic_slice_in_dim(grad, upper * size, size, 0)
            out = jnp.dot(sent, quantized, preferred_element_type=jnp.float32).astype(jnp.bfloat16)
            came = swap(out, "row", n_row, bit)
            total = jnp.dot(kept, quantized, preferred_element_type=jnp.float32) + came.astype(jnp.float32)
            bit //= 2
            while bit:
                size //= 2
                upper = (row // bit) % 2 == 1
                low, high = total[:size], total[size:]
                came = swap(jnp.where(upper, low, high).astype(jnp.bfloat16), "row", n_row, bit)
                total = jnp.where(upper, high, low) + came.astype(jnp.float32)
                bit //= 2
            return total

        products = lax.dot_general(
            own_grad, activations, (((0,), (0,)), ((), ())), preferred_element_type=jnp.float32
        )
        own_total = reduced(own_grad)
        if grads:
            grads[0], quantized, products = lax.optimization_barrier((grads[0], quantized, products))
        running = None
        for k in range(1, n_dp):
            grad = gather_rows(grads[k - 1], "col", n_col)
            total = reduced(grad)
            if running is not None:
                total = total + running.astype(jnp.float32)
            leaving, grad = lax.optimization_barrier((total.astype(jnp.bfloat16), grad))
            running = shift(leaving, "dp", n_dp, 1)
            act = gather_rows(acts[k - 1], "row", n_row)
            products = products + lax.dot_general(
                grad, act, (((0,), (0,)), ((), ())), preferred_element_type=jnp.float32
            )
        if running is not None:
            own_total = own_total + running.astype(jnp.float32)
        products, latent = lax.optimization_barrier((products, weight[0]))
        products = with_layout_constraint(products, Layout((0, 1)))
        _, inside, factor = quantize(latent, own_scales)
        input_grad = own_total.astype(jnp.bfloat16)
        step_rows = lax.psum(jnp.sum(products * factor, axis=1) * grad_factor, "col")
        weight_grad = (products * inside)[None]
        return (input_grad, weight_grad, step_rows[None])

    return shards


MESH = pl.DeviceIdType.MESH


def flipped(position, bit):
    return position + bit * (1 - 2 * lax.rem(position // bit, 2))


def make_kernel(n_dp, n_row, n_col, tokens, own, width):
    quarter = tokens // n_col
    half = tokens // n_row
    piece = 128
    pieces = half // piece
    block = 256
    halves = 2
    g_rows = quarter // halves
    parts = 4
    a_rows = half // parts
    block_pieces = quarter // piece
    factor_scale = 1.0 / (7.0 * width * n_col) ** 0.5
    bits = []
    bit = n_col // 2
    while bit:
        bits.append(bit)
        bit //= 2

    def kernel(act, out_grad, weight, steps, input_grad, weight_grad, step_grad,
               g_buf, a_buf, q_buf, f_buf, p_send, p_recv, c_send, c_recv, w_buf, s_buf, acc, sg_buf, sg_in,
               load_sem, w_sem, gz_send, g_recv, gx_send, az_send, ay_send, a_recv,
               p_ssem, p_rsem, c_ssem, c_rsem, sg_ssem, sg_rsem):
        prod = weight_grad.at[0]
        me = lax.axis_index("dp")
        row = lax.axis_index("row")
        col = lax.axis_index("col")
        partner = 1 - row

        def remote(src, dst, send, recv, where):
            return pltpu.make_async_remote_copy(
                src_ref=src, dst_ref=dst, send_sem=send, recv_sem=recv, device_id=where, device_id_type=MESH
            )

        def rows_of(index, size):
            return pl.ds(pl.multiple_of(index * size, size), size)

        barrier = pltpu.get_barrier_semaphore()
        for k in range(1, n_dp):
            pl.semaphore_signal(barrier, inc=1, device_id={"dp": lax.rem(me + k, n_dp)}, device_id_type=MESH)
        pl.semaphore_signal(barrier, inc=1, device_id={"row": partner}, device_id_type=MESH)
        columns_by = [col]
        for bit in reversed(bits):
            columns_by += [flipped(which, bit) for which in columns_by]
        for which in columns_by[1:]:
            pl.semaphore_signal(barrier, inc=1, device_id={"col": which}, device_id_type=MESH)

        own_columns = pl.ds(pl.multiple_of(me * own, 128), own)
        load_g = pltpu.make_async_copy(out_grad.at[:, own_columns], g_buf.at[me], load_sem.at[0])
        load_a = pltpu.make_async_copy(act, a_buf.at[me], load_sem.at[1])

        def load_w(k):
            return pltpu.make_async_copy(weight.at[0, pl.ds(k * block, block)], w_buf.at[k % 2], w_sem.at[k % 2])

        load_w(0).start()
        load_w(1).start()
        load_g.start()
        load_a.start()
        pl.semaphore_wait(barrier, n_dp - 1 + 1 + n_col - 1)

        def g_span(which, h):
            dealt = lax.rem(which, 2) * (n_col // 2) + which // 2
            return pl.ds(pl.multiple_of(dealt * quarter + h * g_rows, g_rows), g_rows)

        def nth(i):
            return lax.rem(i + col // 2 * block_pieces, pieces)

        def send_g(target, h):
            columns = pl.ds(pl.multiple_of(target * own, 128), own)
            return remote(
                out_grad.at[g_span(col, h), columns], g_buf.at[me, g_span(col, h)],
                gz_send.at[target, h], g_recv.at[me, col, h], {"dp": target},
            )

        upper = me // (n_dp // 2)

        def at(position):
            return position + upper * (n_dp - 1 - 2 * position)

        toward = 1 - 2 * upper
        place = at(me)
        spot = [at(position) for position in range(n_dp)]
        started = ([], [])

        def go(role, make):
            make().start()
            started[role].append(make)

        def give_g(role, target):
            for h in range(halves):
                go(role, lambda h=h: send_g(target, h))

        @pl.when(place == 0)
        def _():
            give_g(0, spot[1])

        @pl.when(place == 1)
        def _():
            give_g(1, spot[2])
            give_g(1, spot[0])

        def a_span(which, h):
            return pl.ds(pl.multiple_of(which * half + h * a_rows, a_rows), a_rows)

        def send_a(source, inward, h, which, slot, own=False):
            span = a_span(which, h)
            return remote(
                act.at[span] if own else a_buf.at[source, span], a_buf.at[source, span],
                az_send.at[slot, inward, h], a_recv.at[source, which, h], {"dp": me + (2 * inward - 1) * toward},
            )

        def swap_a(source, h):
            span = a_span(row, h)
            return remote(
                a_buf.at[source, span], a_buf.at[source, span], ay_send.at[source, h], a_recv.at[source, row, h],
                {"row": partner},
            )

        def arrived_a(source, which, h):
            span = a_span(which, h)
            remote(
                a_buf.at[source, span], a_buf.at[source, span], ay_send.at[source, h], a_recv.at[source, which, h],
                {"row": partner},
            ).wait_recv()

        def give_a(role, inward):
            for h in range(parts):
                go(role, lambda h=h: send_a(me, inward, h, row, me, own=True))

        for k in range(own // 128):
            values = steps[0:1, pl.ds(pl.multiple_of(me * own + k * 128, 128), 128)]
            s_buf[pl.ds(k * 128, 128), :] = jnp.transpose(jnp.broadcast_to(values, (128, 128)))

        n_block = own // block

        for k in range(n_block):
            load_w(k).wait()
            s = jnp.concatenate([s_buf[pl.ds(k * block, block), :]] * (width // 128), axis=1)
            ratio = w_buf[k % 2] / s
            clipped = jnp.clip(ratio, -8.0, 7.0)
            levels = jnp.floor(clipped + 0.5)
            q_buf[pl.ds(k * block, block), :] = (levels * s).astype(jnp.bfloat16)
            f_buf[pl.ds(k * block, block), :] = jnp.where(clipped == ratio, levels - ratio, clipped).astype(jnp.bfloat16)
            if k + 2 < n_block:
                load_w(k + 2).start()
        load_g.wait()

        def dx_tile(d, start, size):
            return jnp.dot(
                g_buf[d, pl.ds(pl.multiple_of(start, size), size), :], q_buf[...], preferred_element_type=jnp.float32
            )

        def partial(d, i):
            part = pl.ds(pl.multiple_of(i * piece, piece), piece)
            return remote(p_send.at[d, part], p_recv.at[d, part], p_ssem.at[d], p_rsem.at[d, i], {"row": partner})

        def send_partials(d, low=0, high=pieces):
            def body(k, carry):
                i = nth(k)
                p_send[d, pl.ds(pl.multiple_of(i * piece, piece), piece), :] = dx_tile(
                    d, partner * half + i * piece, piece
                ).astype(jnp.bfloat16)
                partial(d, i).start()
                return carry

            lax.fori_loop(low, high, body, 0)

        def add_products(d, first=False, last=False):
            def body(k, carry):
                rows = pl.ds(pl.multiple_of(k * block, block), block)
                new = lax.dot_general(
                    g_buf[d, :, rows], a_buf[d], (((0,), (0,)), ((), ())), preferred_element_type=jnp.float32
                )
                if not first:
                    new = new + prod[rows, :]
                if last:
                    factor = f_buf[rows, :].astype(jnp.float32)
                    prod[rows, :] = jnp.where(jnp.abs(factor) < 1.0, new, 0.0)
                    share = new * factor
                    lanes = share[:, 0:128]
                    for j in range(1, width // 128):
                        lanes = lanes + share[:, j * 128:(j + 1) * 128]
                    sg_buf[:, rows] = jnp.sum(jnp.transpose(lanes), axis=0, keepdims=True) * factor_scale
                else:
                    prod[rows, :] = new
                return carry

            lax.fori_loop(0, n_block, body, 0)

        send_partials(me)
        load_a.wait()
        add_products(me, first=True)

        def forward_g(d, differs, bit, slot, h):
            span = g_span(columns_by[differs], h)
            return remote(
                g_buf.at[d, span], g_buf.at[d, span], gx_send.at[d, slot, h], g_recv.at[d, columns_by[differs], h],
                {"col": columns_by[bit]},
            )

        def arrived_g(d, differs, h):
            forward_g(d, differs, bits[0], 0, h).wait_recv()

        def first_g(role, d, then=None):
            for h in range(halves):
                arrived_g(d, 0, h)
                for slot, bit in enumerate(bits):
                    go(role, lambda bit=bit, slot=slot, h=h: forward_g(d, 0, bit, slot, h))
                if h == 0 and then is not None:
                    then()

        def early_g(d):
            for h in range(halves):
                arrived_g(d, 1, h)
            send_partials(d, 0, block_pieces)

        def rest_g(role, d):
            slot, held = len(bits), [0]
            for b, bit in enumerate(bits):
                come = [differs ^ bit for differs in held]
                for differs in come:
                    later = bits[b + 1:]
                    for h in range(halves):
                        if differs != 1:
                            arrived_g(d, differs, h)
                        for j, over in enumerate(later):
                            go(role, lambda differs=differs, over=over, slot=slot + j, h=h: forward_g(d, differs, over, slot, h))
                    slot += len(later)
                held += come
            send_partials(d, block_pieces)

        def chain(d, slot, i, step):
            part = pl.ds(pl.multiple_of(i * piece, piece), piece)
            return remote(c_send.at[d, part], c_recv.at[slot, part], c_ssem.at[d], c_rsem.at[slot, i], {"dp": me + step})

        def own_sum(d, i):
            part = pl.ds(pl.multiple_of(i * piece, piece), piece)
            partial(d, i).wait_recv()
            acc[...] = dx_tile(d, row * half + i * piece, piece) + p_recv[d, part, :].astype(jnp.float32)

        def add_incoming(slot, i):
            part = pl.ds(pl.multiple_of(i * piece, piece), piece)
            remote(
                c_recv.at[slot, part], c_recv.at[slot, part], c_ssem.at[0], c_rsem.at[slot, i], {"row": partner}
            ).wait_recv()
            acc[...] = acc[...] + c_recv[slot, part, :].astype(jnp.float32)

        def pass_step(i, d, inward, first=False, last=False):
            step = toward * (2 * inward - 1)
            slot = d + (1 - step) // 2 * (n_dp - d) if last else d
            part = pl.ds(pl.multiple_of(i * piece, piece), piece)
            own_sum(d, i)
            if not first:
                add_incoming(d, i)
            c_send[d, part, :] = acc[...].astype(jnp.bfloat16)
            chain(d, slot, i, step).start()

        def pass_on(low, high, *jobs):
            def body(i, carry):
                for d, inward, lag, kind in jobs:
                    pass_step(nth(i - lag), d, inward, **kind)
                return carry

            lax.fori_loop(low, high, body, 0)

        def take_a(role, d, onward=(), swaps=tuple(range(parts)), which=tuple(range(parts))):
            for h in which:
                arrived_a(d, row, h)
                for inward in onward:
                    go(role, lambda inward=inward, h=h: send_a(d, inward, h, row, d))
                if h in swaps:
                    go(role, lambda h=h: swap_a(d, h))

        def products_of(d, last=False, skip=()):
            for h in range(parts):
                if h not in skip:
                    arrived_a(d, partner, h)
            add_products(d, last=last)

        def finish():
            def body(k, carry):
                i = nth(k)
                part = pl.ds(pl.multiple_of(i * piece, piece), piece)
                own_sum(me, i)

                @pl.when(me > 0)
                def _():
                    add_incoming(me, i)

                @pl.when(me < n_dp - 1)
                def _():
                    add_incoming(n_dp, i)

                input_grad[part, :] = acc[...].astype(jnp.bfloat16)
                return carry

            lax.fori_loop(0, pieces, body, 0)

        def swap_steps(differs):
            return remote(
                sg_buf, sg_in.at[differs - 1], sg_ssem.at[differs - 1], sg_rsem.at[differs - 1],
                {"col": columns_by[differs]},
            )

        def give_steps(role):
            for differs in range(1, n_col):
                go(role, lambda differs=differs: swap_steps(differs))

        start, end, split = dict(first=True), dict(last=True), pieces // 2
        low, high = tuple(range(parts // 2)), tuple(range(parts // 2, parts))

        @pl.when(place == 0)
        def _():
            r = 0
            first_g(r, spot[1], lambda: give_g(r, spot[2]))
            early_g(spot[1])
            rest_g(r, spot[1])
            give_a(r, 1)

            def meanwhile():
                give_g(r, spot[3])
                take_a(r, spot[1], which=low)

            first_g(r, spot[2], meanwhile)
            early_g(spot[2])
            for h in low:
                go(r, lambda h=h: send_a(me, 1, h, partner, n_dp, own=True))
            rest_g(r, spot[2])
            first_g(r, spot[3])
            early_g(spot[3])
            rest_g(r, spot[3])
            pass_on(0, split, (spot[2], 1, 0, start))
            pass_on(0, pieces - 1, (spot[3], 1, 0, start))
            take_a(r, spot[2])
            pass_on(pieces - 1, pieces, (spot[3], 1, 0, start))
            pass_on(split, pieces, (spot[2], 1, 0, start))
            pass_on(0, pieces, (spot[1], 1, 0, dict(first=True, last=True)))
            take_a(r, spot[3], which=low)
            take_a(r, spot[1], swaps=(), which=high)
            products_of(spot[1])
            take_a(r, spot[3], which=high)
            products_of(spot[2])
            products_of(spot[3], last=True)
            give_steps(r)
            finish()

        @pl.when(place == 1)
        def _():
            r = 1
            first_g(r, spot[0], lambda: give_a(r, 0))
            first_g(r, spot[2])
            give_g(r, spot[3])
            early_g(spot[0])
            early_g(spot[2])
            rest_g(r, spot[0])
            first_g(r, spot[3])
            early_g(spot[3])
            rest_g(r, spot[2])
            give_a(r, 1)
            rest_g(r, spot[3])
            for h in high:
                go(r, lambda h=h: send_a(me, 0, h, partner, n_dp, own=True))
            take_a(r, spot[0], (1,), swaps=high)
            take_a(r, spot[2], (0,))
            take_a(r, spot[3], (0,), which=low)
            pass_on(0, split, (spot[2], 1, 0, end))
            products_of(spot[0])
            take_a(r, spot[3], (0,), which=high)
            pass_on(0, 1, (spot[3], 1, 0, {}))
            pass_on(1, split, (spot[3], 1, 0, {}))
            products_of(spot[2])
            pass_on(split, pieces, (spot[3], 1, 0, {}), (spot[0], 0, split, end))
            pass_on(split, pieces - 1, (spot[0], 0, 0, end))
            pass_on(split, pieces, (spot[2], 1, 0, end))
            pass_on(pieces - 1, pieces, (spot[0], 0, 0, end))
            products_of(spot[3], last=True)
            give_steps(r)
            finish()

        for differs in range(1, n_col):
            swap_steps(differs).wait_recv()
        total = sg_buf[...]
        for differs in range(1, n_col):
            total = total + sg_in[differs - 1]
        step_grad[...] = total

        for role in range(2):
            @pl.when(place == role)
            def _():
                for make in started[role]:
                    make().wait_send()

        def drain(d, carry):
            remote(p_send.at[d], p_send.at[d], p_ssem.at[d], p_rsem.at[d, 0], {"row": partner}).wait_send()

            @pl.when(me != d)
            def _():
                remote(c_send.at[d], c_send.at[d], c_ssem.at[d], c_rsem.at[d, 0], {"row": partner}).wait_send()

            return carry

        lax.fori_loop(0, n_dp, drain, 0)
    scratch = [
        pltpu.VMEM((n_dp, tokens, own), jnp.bfloat16),
        pltpu.VMEM((n_dp, tokens, width), jnp.bfloat16),
        pltpu.VMEM((own, width), jnp.bfloat16),
        pltpu.VMEM((own, width), jnp.bfloat16),
        pltpu.VMEM((n_dp, half, width), jnp.bfloat16),
        pltpu.VMEM((n_dp, half, width), jnp.bfloat16),
        pltpu.VMEM((n_dp, half, width), jnp.bfloat16),
        pltpu.VMEM((n_dp + 1, half, width), jnp.bfloat16),
        pltpu.VMEM((2, block, width), jnp.float32),
        pltpu.VMEM((own, 128), jnp.float32),
        pltpu.VMEM((piece, width), jnp.float32),
        pltpu.VMEM((1, own), jnp.float32),
        pltpu.VMEM((n_col - 1, 1, own), jnp.float32),
        pltpu.SemaphoreType.DMA((2,)),
        pltpu.SemaphoreType.DMA((2,)),
        pltpu.SemaphoreType.DMA((n_dp, halves)),
        pltpu.SemaphoreType.DMA((n_dp, n_col, halves)),
        pltpu.SemaphoreType.DMA((n_dp, n_col - 1, halves)),
        pltpu.SemaphoreType.DMA((n_dp + 1, 2, parts)),
        pltpu.SemaphoreType.DMA((n_dp, parts)),
        pltpu.SemaphoreType.DMA((n_dp, n_row, parts)),
        pltpu.SemaphoreType.DMA((n_dp,)),
        pltpu.SemaphoreType.DMA((n_dp, pieces)),
        pltpu.SemaphoreType.DMA((n_dp,)),
        pltpu.SemaphoreType.DMA((n_dp + 1, pieces)),
        pltpu.SemaphoreType.DMA((n_col - 1,)),
        pltpu.SemaphoreType.DMA((n_col - 1,)),
    ]
    anywhere = pl.BlockSpec(memory_space=pl.ANY)
    inside = pl.BlockSpec(memory_space=pltpu.VMEM)
    return pl.pallas_call(
        kernel,
        out_shape=(
            pltpu.VMEM((half, width), jnp.bfloat16),
            pltpu.VMEM((1, own, width), jnp.float32),
            pltpu.VMEM((1, own), jnp.float32),
        ),
        in_specs=[anywhere, anywhere, anywhere, inside],
        out_specs=(inside, inside, inside),
        scratch_shapes=scratch,
        compiler_params=pltpu.CompilerParams(collective_id=0, has_side_effects=True, vmem_limit_bytes=55 * 2**20),
        name="backward",
    )


def leave(input_grad, weight_grad, step_grad):
    held = (input_grad, weight_grad, step_grad)
    cuts = 8
    rows = weight_grad.shape[1] // cuts

    def kernel(a, b, c, a_out, b_out, c_out, sems):
        copies = [pltpu.make_async_copy(a, a_out, sems.at[cuts]), pltpu.make_async_copy(c, c_out, sems.at[cuts + 1])]
        for k in range(cuts):
            span = pl.ds(k * rows, rows)
            copies.append(pltpu.make_async_copy(b.at[:, span], b_out.at[:, span], sems.at[k]))
        for copy in copies:
            copy.start()
        for copy in copies:
            copy.wait()

    return pl.pallas_call(
        kernel,
        out_shape=tuple(jax.ShapeDtypeStruct(x.shape, x.dtype) for x in held),
        in_specs=[pl.BlockSpec(memory_space=pltpu.VMEM)] * len(held),
        out_specs=tuple(pl.BlockSpec(memory_space=pl.ANY) for _ in held),
        scratch_shapes=[pltpu.SemaphoreType.DMA((cuts + 2,))],
        compiler_params=pltpu.CompilerParams(vmem_limit_bytes=2**20),
        name="leave",
    )(*(pltpu.with_memory_space_constraint(x, pltpu.VMEM) for x in held))


def fits(n_dp, n_row, n_col, activations, weight):
    tokens, width = activations.shape
    own = weight.shape[1]
    return (
        n_dp == 4 and n_row == 2 and n_col > 1 and n_col & (n_col - 1) == 0
        and own % 256 == 0 and width % 128 == 0 and tokens % (256 * n_row) == 0 and tokens % (128 * n_col) == 0
        and n_dp * tokens * (own + width) <= 12 * 2**20
    )


def solution(mesh):
    n_dp, n_row, n_col = mesh.shape["dp"], mesh.shape["row"], mesh.shape["col"]
    in_specs = (P("dp", "col"), P("dp", "row"), P("row", "dp", "col"), P("row", None))
    out_specs = (P(("dp", "row"), "col"), P("row", "dp", "col"), P("row", "dp"))
    general = make_shards(n_dp, n_row, n_col)

    def shards(activations, out_grad, weight, step_size):
        if not fits(n_dp, n_row, n_col, activations, weight):
            return general(activations, out_grad, weight, step_size)
        tokens, width = activations.shape
        call = make_kernel(n_dp, n_row, n_col, tokens, weight.shape[1], width)
        return leave(*call(activations, out_grad, weight, step_size))

    return jax.shard_map(shards, mesh=mesh, in_specs=in_specs, out_specs=out_specs, check_vma=False)
```
